256 devices in a mesh: pulse: 8 (over y_lo, x), tile: 32 (over z, y_hi, core).
Axes of the slice: x: 4, y: 4 (y_hi: 2, y_lo: 2; y = y_hi * 2 + y_lo), z: 8, core: 2. Of those that a mesh axis runs over, the one named last changes fastest.
Arguments:
- pulses: bfloat16 [4096, 2, 32768], P(None, None, ('pulse', 'tile')), may hold values from -6 to 6
- steering: bfloat16 [2, 128, 128], replicated, may hold values from -0.375 to 0.375
- merge_re: bfloat16 [3, 256, 256], replicated, may hold values from -0.25 to 0.25
- merge_im: bfloat16 [3, 256, 256], replicated, may hold values from -0.25 to 0.25
- range_shift: int32 [3, 2, 128], replicated, may hold values from -8 to 8
- image_map: bfloat16 [8, 32, 2, 128, 512], P('pulse', 'tile'), may hold values from -0.0234375 to 0.0234375
Outputs:
- image: float32 [4096, 1024], P(('pulse', 'tile'))
The draws below stay inside these ranges and needn't reach their ends.
All inputs are finite; a program needn't handle non-finite values.
Results may differ from the reference program's by a relative error of at most 0.0057.
Values may be sent and summed in bfloat16 or wider, within the bound.
A program may use at most 64 MiB of HBM per device.

```python
import jax
import jax.numpy as jnp
import numpy as np
from jax import lax

R = 4096
PD = 128
K = 128
X = 512
LEVELS = 3
SHIFT = 8
GROUPS = 8
SUBS = 32
N_PULSE = 8
N_TILE = 32
DEVICES = 256


def place_ends(array, own_key, low, largest):
    place = [jax.random.randint(jax.random.fold_in(own_key, axis), (), 0, length) for axis, length in enumerate(array.shape)]
    main_axis = array.shape.index(max(array.shape))
    neighbour = place[:main_axis] + [(place[main_axis] + 1) % array.shape[main_axis]] + place[main_axis + 1:]
    return array.at[tuple(place)].set(low).at[tuple(neighbour)].set(largest)


def levels(rng, shape, split, least, high):
    loudness, own = 1.0, jax.random.fold_in(rng, 6)
    for axis_at, blocks in split:
        steps = jnp.exp(jax.random.uniform(jax.random.fold_in(own, axis_at), (blocks,), jnp.float32, least / len(split), high / len(split)))
        loudness = loudness * jnp.repeat(steps, shape[axis_at] // blocks).reshape([-1 if axis == axis_at else 1 for axis in range(len(shape))])
    return loudness


def scatter_about(stream_key, shape, spread, limit, cuts=(), kind=jnp.bfloat16):
    entries = jax.random.normal(stream_key, shape, jnp.float32) * spread
    if len(cuts) > 0:
        entries = levels(stream_key, shape, cuts, -0.22, 0.18) * entries
    return jnp.clip(entries, min=-limit, max=limit).astype(kind)


def setup_inputs(seed: int = 0) -> dict:
    key_list = jax.random.split(jax.random.key(seed), 7)
    pulses = scatter_about(key_list[0], (R, 2, PD * DEVICES), 1.0, 6.0, ((2, 256),))
    steering = scatter_about(key_list[1], (2, PD, K), (2 * PD) ** -0.5, 0.375)
    merge_re = scatter_about(key_list[2], (LEVELS, 2 * K, 2 * K), (4 * K) ** -0.5, 0.25)
    merge_im = scatter_about(key_list[3], (LEVELS, 2 * K, 2 * K), (4 * K) ** -0.5, 0.25)
    range_shift = place_ends(jax.random.randint(key_list[4], (LEVELS, 2, K), 0 - SHIFT, SHIFT + 1), jax.random.fold_in(key_list[4], 1), 0 - SHIFT, SHIFT).astype(jnp.int32)
    image_map = scatter_about(key_list[5], (GROUPS, SUBS, 2, K, X), (2 * K * DEVICES) ** -0.5, 0.0234375, ((0, 8), (1, 32)))
    return {"pulses": pulses, "steering": steering, "merge_re": merge_re, "merge_im": merge_im, "range_shift": range_shift, "image_map": image_map}


def complex_block(real_part, imag_part):
    upper_half = jnp.concatenate([real_part, imag_part], axis=1)
    lower_half = jnp.concatenate([-imag_part, real_part], axis=1)
    return jnp.concatenate([upper_half, lower_half], axis=0)


def shift_rows(beam_rows, shift_table):
    range_rows = beam_rows.shape[0]
    doubled = jnp.concatenate([shift_table, shift_table]).astype(jnp.int32)
    source = jnp.arange(range_rows, dtype=jnp.int32)[:, None] + doubled[None, :]
    inside = (source >= 0) & (source < range_rows)
    picked = jnp.take_along_axis(beam_rows, jnp.clip(source, 0, range_rows - 1), axis=0)
    return jnp.where(inside, picked, jnp.zeros_like(picked))


def reference(pulses, steering, merge_re, merge_im, range_shift, image_map):
    steer_block = complex_block(steering[0], steering[1]).astype(jnp.float32)
    shaped = pulses.reshape(R, 2, N_PULSE, N_TILE, PD).transpose(2, 3, 0, 1, 4).reshape(N_PULSE, N_TILE, R, 2 * PD)
    level_blocks = []
    for merge_level in range(LEVELS):
        chosen = []
        for half_bit in range(2):
            weight_re = merge_re[merge_level][:, half_bit * K:(half_bit + 1) * K]
            weight_im = merge_im[merge_level][:, half_bit * K:(half_bit + 1) * K]
            chosen.append(complex_block(weight_re, weight_im))
        level_blocks.append(jnp.stack(chosen))

    def group_term(running_sum, inputs):
        pulse_block, group_maps = inputs
        current = jnp.einsum("srp,pk->srk", pulse_block.astype(jnp.float32), steer_block).astype(jnp.bfloat16)
        for merge_level in range(LEVELS):
            partner_index = np.arange(N_TILE) ^ (1 << merge_level)
            halves = (np.arange(N_TILE) >> merge_level) & 1
            partner = current[partner_index]
            is_upper = jnp.asarray(halves == 1)[:, None, None]
            lower_src = jnp.where(is_upper, partner, current)
            upper_src = jnp.where(is_upper, current, partner)
            shifted_lower = jax.vmap(shift_rows, (0, None))(lower_src, range_shift[merge_level, 0])
            shifted_upper = jax.vmap(shift_rows, (0, None))(upper_src, range_shift[merge_level, 1])
            combined = jnp.concatenate([shifted_lower[..., :K], shifted_upper[..., :K], shifted_lower[..., K:], shifted_upper[..., K:]], axis=-1)
            per_sub = level_blocks[merge_level][halves]
            current = jnp.einsum("srk,skn->srn", combined.astype(jnp.float32), per_sub.astype(jnp.float32)).astype(jnp.bfloat16)
        map_blocks = jax.vmap(complex_block)(group_maps[:, 0], group_maps[:, 1])
        contribution = jnp.einsum("srk,skx->rx", current.astype(jnp.float32), map_blocks.astype(jnp.float32))
        return running_sum + contribution, None

    start_sum = jnp.zeros((R, 2 * X), jnp.float32)
    image, _ = lax.scan(group_term, start_sum, (shaped, image_map))
    return image
```

```python
import functools

import jax
import jax.numpy as jnp
from jax import lax
from jax.experimental import pallas as pl
from jax.experimental.pallas import tpu as pltpu
from jax.sharding import PartitionSpec as P

MESH = pl.DeviceIdType.MESH
F32 = jnp.float32
BF16 = jnp.bfloat16
HALO = 32
CHUNK = 256
WIDTH = 256
STREAMS = (("x", 0), ("y", 512), ("x", 256), ("y", 768))


def complex_block(real_part, imag_part):
    upper_half = jnp.concatenate([real_part, imag_part], axis=1)
    lower_half = jnp.concatenate([-imag_part, real_part], axis=1)
    return jnp.concatenate([upper_half, lower_half], axis=0)


def shifted(rows, table):
    groups = rows.shape[0] // 8
    at = lax.broadcasted_iota(jnp.int32, (8, 128), 0) + table
    index = jnp.bitwise_and(at + 8, 7)
    below, above = at < 0, at > 7
    picked = [
        jnp.take_along_axis(rows[8 * g : 8 * g + 8], index, axis=0, mode="promise_in_bounds")
        for g in range(groups)
    ]
    return jnp.concatenate(
        [
            jnp.where(below, picked[g - 1], jnp.where(above, picked[g + 1], picked[g]))
            for g in range(1, groups - 1)
        ],
        axis=0,
    )


def front_kernel(place, own_t, own_m, own_b, oth_t, oth_m, oth_b, re_ref, im_ref, table_ref, out_ref, w0, w1, buf0, buf1, buf2):
    g = pl.program_id(0)
    core, y_hi, z_lo = place[0], place[1], place[2]
    other = 1 - core

    @pl.when(g == 0)
    def _():
        for side, u in ((0, core), (1, other)):
            for h in range(2):
                a = re_ref[0, pl.ds(pl.multiple_of(u * 128, 128), 128), h * 128 : h * 128 + 128]
                b = im_ref[0, pl.ds(pl.multiple_of(u * 128, 128), 128), h * 128 : h * 128 + 128]
                r, c = side * 256, h * 256
                w0[r : r + 128, c : c + 128] = a
                w0[r : r + 128, c + 128 : c + 256] = b
                w0[r + 128 : r + 256, c : c + 128] = -b
                w0[r + 128 : r + 256, c + 128 : c + 256] = a
        for h in range(2):
            a = re_ref[1, pl.ds(pl.multiple_of(y_hi * 128, 128), 128), h * 128 : h * 128 + 128]
            b = im_ref[1, pl.ds(pl.multiple_of(y_hi * 128, 128), 128), h * 128 : h * 128 + 128]
            c = h * 256
            w1[0:128, c : c + 128] = a
            w1[0:128, c + 128 : c + 256] = b
            w1[128:256, c : c + 128] = -b
            w1[128:256, c + 128 : c + 256] = a

    first = jnp.logical_and(g == 0, core == 0)
    last = jnp.logical_and(g == pl.num_programs(0) - 1, core == 1)
    keep_top = jnp.where(first, 0.0, 1.0).astype(F32)
    keep_bottom = jnp.where(last, 0.0, 1.0).astype(F32)
    for side, (t, m, b) in enumerate(((own_t, own_m, own_b), (oth_t, oth_m, oth_b))):
        cols = slice(side * 256, side * 256 + 256)
        buf0[0:HALO, cols] = t[0].astype(F32) * keep_top
        buf0[HALO : HALO + CHUNK, cols] = m[0].astype(F32)
        buf0[HALO + CHUNK :, cols] = b[0].astype(F32) * keep_bottom

    parts = []
    for side, u in ((0, core), (1, other)):
        table = table_ref[0, pl.ds(u, 1), :]
        for half in range(2):
            c = side * 256 + half * 128
            parts.append(shifted(buf0[8 : 16 + 288 + 8, c : c + 128], table).astype(BF16))
    merged = jnp.dot(jnp.concatenate(parts, axis=1), w0[...], preferred_element_type=F32).astype(BF16)
    buf1[0:16, :] = merged[0:16].astype(F32) * keep_top
    buf1[16:272, :] = merged[16:272].astype(F32)
    buf1[272:288, :] = merged[272:288].astype(F32) * keep_bottom

    table = table_ref[1, pl.ds(y_hi, 1), :]
    for s in range(2):
        part = jnp.concatenate(
            [shifted(buf1[:, s * 256 + 128 * k : s * 256 + 128 * k + 128], table).astype(BF16) for k in range(2)], axis=1
        )
        merged = jnp.dot(part, w1[...], preferred_element_type=F32).astype(BF16)
        cols = slice(s * 512, s * 512 + 512)
        buf2[0:8, cols] = merged[0:8].astype(F32) * keep_top
        buf2[8:264, cols] = merged[8:264].astype(F32)
        buf2[264:272, cols] = merged[264:272].astype(F32) * keep_bottom

    table = table_ref[2, pl.ds(z_lo, 1), :]
    for k in range(8):
        moved = shifted(buf2[:, 128 * k : 128 * k + 128], table).astype(BF16)
        out_ref[0, 0, :, :, :, 128 * k : 128 * k + 128] = moved.reshape(4, 2, 32, 128)


def front(place, own, oth, merge_re, merge_im, range_shift):
    main = own.reshape(16, 256, 256), oth.reshape(16, 256, 256)
    edge = own.reshape(128, 32, 256), oth.reshape(128, 32, 256)
    top = pl.BlockSpec((1, 32, 256), lambda g, s: (jnp.maximum(8 * (2 * g + s[0]) - 1, 0), 0, 0))
    mid = pl.BlockSpec((1, 256, 256), lambda g, s: (2 * g + s[0], 0, 0))
    bot = pl.BlockSpec((1, 32, 256), lambda g, s: (jnp.minimum(8 * (2 * g + s[0]) + 8, 127), 0, 0))
    whole = pl.BlockSpec(memory_space=pltpu.VMEM)
    return pl.pallas_call(
        front_kernel,
        grid_spec=pltpu.PrefetchScalarGridSpec(
            num_scalar_prefetch=1,
            grid=(8,),
            in_specs=[top, mid, bot, top, mid, bot, whole, whole, whole],
            out_specs=pl.BlockSpec((1, 1, 4, 2, 32, 1024), lambda g, s: (g // 4, g % 4, 0, 0, 0, 0)),
            scratch_shapes=[
                pltpu.VMEM((512, 512), BF16),
                pltpu.VMEM((256, 512), BF16),
                pltpu.VMEM((CHUNK + 2 * HALO, 512), F32),
                pltpu.VMEM((288, 512), F32),
                pltpu.VMEM((272, 1024), F32),
            ],
        ),
        out_shape=jax.ShapeDtypeStruct((2, 4, 4, 2, 32, 1024), BF16),
        cost_estimate=pl.CostEstimate(flops=2_600_000_000, bytes_accessed=9_000_000, transcendentals=0),
        name="front",
    )(place, edge[0], main[0], edge[0], edge[1], main[1], edge[1], merge_re, merge_im, range_shift)


def image_kernel(lhs, maps, out_ref, rhs, acc_x, acc_y, fin, s1, r1, s2, r2, s3, r3, ss1, rs1, ss2, rs2, ss3, rs3):
    pulse, tile = lax.axis_index("pulse"), lax.axis_index("tile")
    y_lo, x = pulse // 4, pulse % 4
    z, y_hi, core = tile // 4, (tile // 2) % 2, tile % 2
    y = 2 * y_hi + y_lo

    def along_x(step):
        return (4 * y_lo + (x + step) % 4, tile)

    def along_y(step):
        to = (y + step) % 4
        return (4 * (to % 2) + x, 4 * z + 2 * (to // 2) + core)

    def along_z(to, its_core):
        return (pulse, 4 * to + 2 * y_hi + its_core)

    def z_other(to, its_core):
        return jnp.logical_or(to != z, its_core != core)

    barrier = pltpu.get_barrier_semaphore()
    for step in (1, 3):
        pl.semaphore_signal(barrier, inc=1, device_id=along_x(step), device_id_type=MESH)
        pl.semaphore_signal(barrier, inc=1, device_id=along_y(step), device_id_type=MESH)
    for off in range(16):
        to, its_core = (z + off // 2) % 8, (core + off % 2) % 2
        if off:
            pl.semaphore_signal(barrier, inc=1, device_id=along_z(to, its_core), device_id_type=MESH)

    for t in range(4):
        re, im = maps[t, 0], maps[t, 1]
        rhs[t * 256 : t * 256 + 128, 0:512] = re
        rhs[t * 256 : t * 256 + 128, 512:1024] = im
        rhs[t * 256 + 128 : t * 256 + 256, 0:512] = -im
        rhs[t * 256 + 128 : t * 256 + 256, 512:1024] = re

    def image_half(n, dest, h):
        kind, col = STREAMS[n]
        if kind == "x":
            rows = lhs[h, dest].reshape(256, 1024)
        else:
            rows = lhs[dest % 2, 2 * h : 2 * h + 2, :, dest // 2].reshape(256, 1024)
        return jnp.dot(rows, rhs[:, col : col + WIDTH], preferred_element_type=F32)

    def total_half(n, dest, h):
        if STREAMS[n][0] == "x":
            return acc_x[n // 2, dest % 2, h, :, dest // 2].reshape(64, WIDTH)
        return acc_y[n // 2, dest // 2, dest % 2, h].reshape(64, WIDTH)

    def ring(n, phase):
        kind = STREAMS[n][0]
        use_x = (kind == "x") == (phase == 1)
        here, to = (x, along_x) if use_x else (y, along_y)
        half = image_half if phase == 1 else total_half
        send, recv, ssem, rsem = (s1, r1, ss1, rs1) if phase == 1 else (s2, r2, ss2, rs2)
        return here, to, half, send, recv, ssem, rsem

    SLOTS = ((2, 0, 1), (2, 1, 3), (1, 1, 1), (3, 0, 3), (1, 0, 1), (3, 1, 3))

    def copy(n, phase, slot):
        here, to, half, send, recv, ssem, rsem = ring(n, phase)
        return pltpu.make_async_remote_copy(
            src_ref=send.at[n, slot],
            dst_ref=recv.at[n, slot],
            send_sem=ssem.at[n, slot],
            recv_sem=rsem.at[n, slot],
            device_id=to(SLOTS[slot][2]),
            device_id_type=MESH,
        )

    def open_ring(n, phase, wait_barrier=False):
        here, to, half, send, recv, ssem, rsem = ring(n, phase)
        for slot in range(4):
            ahead, h, _ = SLOTS[slot]
            send[n, slot] = half(n, (here + ahead) % 4, h).astype(BF16)
            if slot == 0 and wait_barrier:
                pl.semaphore_wait(barrier, 19)
            copy(n, phase, slot).start()

    def relay_ring(n, phase):
        here, to, half, send, recv, ssem, rsem = ring(n, phase)
        for slot in (4, 5):
            ahead, h, _ = SLOTS[slot]
            mine = half(n, (here + ahead) % 4, h)
            copy(n, phase, slot - 4).wait_recv()
            send[n, slot] = (mine + recv[n, slot - 4].astype(F32)).astype(BF16)
            copy(n, phase, slot).start()

    def close_ring(n, phase):
        here, to, half, send, recv, ssem, rsem = ring(n, phase)
        for h, slots in ((0, (3, 4)), (1, (2, 5))):
            value = half(n, here, h)
            for slot in slots:
                copy(n, phase, slot).wait_recv()
                value = value + recv[n, slot].astype(F32)
            if phase == 2:
                fin[n, 2 * h : 2 * h + 2] = value.reshape(2, 32, WIDTH)
            elif STREAMS[n][0] == "x":
                acc_x[n // 2, h] = value.reshape(2, 2, 2, 32, WIDTH)
            else:
                acc_y[n // 2, h] = value.reshape(2, 2, 2, 32, WIDTH)

    def z_copy(n, i, c, to, its_core, src_z):
        return pltpu.make_async_remote_copy(
            src_ref=s3.at[n, i, c],
            dst_ref=r3.at[n, src_z],
            send_sem=ss3.at[n, i, c],
            recv_sem=rs3.at[n, src_z],
            device_id=along_z(to, its_core),
            device_id_type=MESH,
        )

    def open_z(n):
        for i in range(4):
            for c in range(2):
                s3[n, i, c] = fin[n, i, 16 * c : 16 * c + 16].astype(BF16)
        for i in range(4):
            for c in range(2):
                to = 4 * core + i

                @pl.when(z_other(to, c))
                def _():
                    z_copy(n, i, c, to, c, z).start()

                @pl.when(jnp.logical_not(z_other(to, c)))
                def _():
                    r3[n, z] = s3[n, i, c]

    def close_z(n):
        col = STREAMS[n][1]
        source_core = z // 4
        value = jnp.zeros((16, WIDTH), F32)
        for off in range(8):
            src = (z + off) % 8

            @pl.when(z_other(src, source_core))
            def _():
                z_copy(n, 0, 0, (z + 1) % 8, core, src).wait_recv()

        for src in range(8):
            value = value + r3[n, src].astype(F32)
        out_ref[:, col : col + WIDTH] = value

    open_ring(0, 1, True)
    open_ring(1, 1)
    relay_ring(0, 1)
    relay_ring(1, 1)
    open_ring(2, 1)
    open_ring(3, 1)
    close_ring(0, 1)
    open_ring(0, 2)
    close_ring(1, 1)
    open_ring(1, 2)
    relay_ring(0, 2)
    relay_ring(1, 2)
    relay_ring(2, 1)
    relay_ring(3, 1)
    close_ring(0, 2)
    open_z(0)
    close_ring(1, 2)
    open_z(1)
    close_ring(2, 1)
    open_ring(2, 2)
    close_ring(3, 1)
    open_ring(3, 2)
    relay_ring(2, 2)
    relay_ring(3, 2)
    close_ring(2, 2)
    open_z(2)
    close_ring(3, 2)
    open_z(3)
    for n in range(4):
        close_z(n)
    for n in range(4):
        for slot in range(6):
            copy(n, 1, slot).wait_send()
            copy(n, 2, slot).wait_send()
        for i in range(4):
            for c in range(2):
                to = 4 * core + i

                @pl.when(z_other(to, c))
                def _():
                    z_copy(n, i, c, to, c, z).wait_send()


def image_sum(lhs, maps):
    vmem = pl.BlockSpec(memory_space=pltpu.VMEM)
    dma = pltpu.SemaphoreType.DMA
    return pl.pallas_call(
        image_kernel,
        out_shape=jax.ShapeDtypeStruct((16, 1024), F32),
        in_specs=[vmem, vmem],
        out_specs=vmem,
        scratch_shapes=[
            pltpu.VMEM((1024, 1024), BF16),
            pltpu.VMEM((2, 2, 2, 2, 2, 32, WIDTH), F32),
            pltpu.VMEM((2, 2, 2, 2, 2, 32, WIDTH), F32),
            pltpu.VMEM((4, 4, 32, WIDTH), F32),
            pltpu.VMEM((4, 6, 256, WIDTH), BF16),
            pltpu.VMEM((4, 6, 256, WIDTH), BF16),
            pltpu.VMEM((4, 6, 64, WIDTH), BF16),
            pltpu.VMEM((4, 6, 64, WIDTH), BF16),
            pltpu.VMEM((4, 4, 2, 16, WIDTH), BF16),
            pltpu.VMEM((4, 8, 16, WIDTH), BF16),
            dma((4, 6)),
            dma((4, 6)),
            dma((4, 6)),
            dma((4, 6)),
            dma((4, 4, 2)),
            dma((4, 8)),
        ],
        compiler_params=pltpu.CompilerParams(
            collective_id=0, has_side_effects=True, vmem_limit_bytes=48 * 1024 * 1024
        ),
        cost_estimate=pl.CostEstimate(flops=4_300_000_000, bytes_accessed=6_000_000, transcendentals=0),
        name="image_sum",
    )(lhs, maps)


def swap(value, mask):
    return lax.ppermute(value, "tile", [(t, t ^ mask) for t in range(lax.axis_size("tile"))])


def body(pulses, steering, merge_re, merge_im, range_shift, image_map):
    tile = lax.axis_index("tile")
    core, y_hi, z_lo = tile % 2, (tile // 2) % 2, (tile // 4) % 2
    own_map = image_map.reshape(256, 512)
    oth_map = swap(own_map, 4)
    stack = jnp.concatenate([own_map, oth_map], axis=0)

    def weights(h):
        a = lax.dynamic_slice(merge_re[2], (z_lo * 128, h * 128), (128, 128))
        b = lax.dynamic_slice(merge_im[2], (z_lo * 128, h * 128), (128, 128))
        return complex_block(a, -b)

    fold = jnp.concatenate([weights(z_lo), weights(1 - z_lo)], axis=1)
    mine = jnp.dot(fold, stack, preferred_element_type=F32).astype(BF16)
    far = swap(mine, 2)
    pair = jnp.stack([mine, far])
    near = swap(pair, 1)
    both = jnp.stack([pair, near])
    both = jnp.where(core == 1, both[::-1], both)
    both = jnp.where(y_hi == 1, both[:, ::-1], both)
    maps = both.reshape(4, 2, 128, 512)

    rows = pulses.reshape(pulses.shape[0], -1)
    own = jnp.dot(rows, complex_block(steering[0], steering[1]), preferred_element_type=F32).astype(BF16)
    oth = swap(own, 1)
    place = jnp.stack([core, y_hi, z_lo]).astype(jnp.int32)
    lhs = front(place, own, oth, merge_re, merge_im, range_shift)
    return image_sum(lhs, maps)


def solution(mesh):
    placed = (
        P(None, None, ("pulse", "tile")),
        P(),
        P(),
        P(),
        P(),
        P("pulse", "tile", None, None, None),
    )
    return jax.shard_map(
        body, mesh=mesh, in_specs=placed, out_specs=P(("pulse", "tile"), None), check_vma=False
    )
```

```python
import jax
import jax.numpy as jnp
from jax import lax
from jax.experimental import pallas as pl
from jax.experimental.pallas import tpu as pltpu
from jax.sharding import PartitionSpec as P

MESH = pl.DeviceIdType.MESH
F32 = jnp.float32
BF16 = jnp.bfloat16
WIDTH = 256
STREAMS = ("x", "y", "x", "y")
TOWARD = (1, 3, 1, 3, 1, 3)


def dot(a, b):
    return jnp.dot(a, b, preferred_element_type=F32)


def shifted(rows, table):
    groups = rows.shape[0] // 8
    at = lax.broadcasted_iota(jnp.int32, (8, 128), 0) + table
    index = jnp.bitwise_and(at + 8, 7)
    below, above = at < 0, at > 7
    picked = [
        jnp.take_along_axis(rows[8 * g : 8 * g + 8], index, axis=0, mode="promise_in_bounds")
        for g in range(groups)
    ]
    return jnp.concatenate(
        [
            jnp.where(below, picked[g - 1], jnp.where(above, picked[g + 1], picked[g]))
            for g in range(1, groups - 1)
        ],
        axis=0,
    )


def kernel(
    pulses, steer_in, re_in, im_in, table_in, map_in, out_ref,
    steer, re_ref, im_ref, table_ref, own_map, pbuf, ws, w0, w1, w2, qbuf, buf0, buf1, buf2, lhs, mbuf, nbuf, rhs, held, total,
    s1, r1, sa2, ra2, sb2, rb2, sa3, ra3, sb3, rb3, small,
    ins, po, ps, pr, ms, mr, ns, nr, ss1, rs1, ss2, rs2, ss3, rs3,
):
    pulse, tile = lax.axis_index("pulse"), lax.axis_index("tile")
    y_lo, x = pulse // 4, pulse % 4
    z, y_hi, core = tile // 4, (tile // 2) % 2, tile % 2
    y, z_lo, other = 2 * y_hi + y_lo, z % 2, 1 - core

    def along_x(step):
        return (4 * y_lo + (x + step) % 4, tile)

    def along_y(step):
        to = (y + step) % 4
        return (4 * (to % 2) + x, 4 * z + 2 * (to // 2) + core)

    def along_z(to, its_core):
        return (pulse, 4 * to + 2 * y_hi + its_core)

    def z_other(to, its_core):
        return jnp.logical_or(to != z, its_core != core)

    z_mate = along_z(z + 1 - 2 * z_lo, core)
    core_mate = along_z(z, other)
    y_mate = along_y(2)

    fetches = [
        pltpu.make_async_copy(src, dst, ins.at[i])
        for i, (src, dst) in enumerate(
            ((map_in, own_map), (steer_in, steer), (re_in, re_ref), (im_in, im_ref), (table_in, table_ref))
        )
    ]
    for fetch in fetches:
        fetch.start()

    barrier = pltpu.get_barrier_semaphore()
    for step in (1, 2, 3):
        pl.semaphore_signal(barrier, inc=1, device_id=along_x(step), device_id_type=MESH)
        pl.semaphore_signal(barrier, inc=1, device_id=along_y(step), device_id_type=MESH)
    for off in range(1, 16):
        mate = along_z((z + off // 2) % 8, (core + off % 2) % 2)
        pl.semaphore_signal(barrier, inc=1, device_id=mate, device_id_type=MESH)

    def rows_of(side, g, c):
        wanted = g * 1024 + c * 512 - 64
        start = jnp.clip(wanted, 0, pulses.shape[0] - 640)
        at = 64 + start - wanted
        return (
            pulses.at[pl.ds(pl.multiple_of(start, 64), 640)],
            pbuf.at[side, g, pl.ds(pl.multiple_of(at, 64), 640)],
        )

    def own_copy(g):
        src, dst = rows_of(0, g, core)
        return pltpu.make_async_copy(src, dst, po.at[g])

    def mate_copy(g):
        src, dst = rows_of(1, g, other)
        return pltpu.make_async_remote_copy(
            src_ref=src, dst_ref=dst, send_sem=ps.at[0], recv_sem=pr.at[g], device_id=core_mate, device_id_type=MESH
        )

    def drain(ref, sem):
        pltpu.make_async_copy(ref, ref, sem).wait()

    def order(k):
        ahead = jnp.where(k < 2, 2, jnp.where(k < 4, 1, jnp.where(k < 6, 3, 0)))
        return 4 * (k % 2) + (x + ahead) % 4

    @pl.loop(0, 8)
    def _(k):
        own_copy(order(k)).start()

    zeros = jnp.zeros((64, 128), BF16)

    @pl.when(core == 0)
    def _():
        pbuf[0, 0, 64:128] = zeros
        pbuf[1, 0, 64:128] = zeros

    @pl.when(core == 1)
    def _():
        pbuf[0, 7, 640:704] = zeros
        pbuf[1, 7, 640:704] = zeros

    def map_copy(q):
        return pltpu.make_async_remote_copy(
            src_ref=own_map.at[:, q * 128 : q * 128 + 128],
            dst_ref=mbuf.at[q],
            send_sem=ms.at[0],
            recv_sem=mr.at[q],
            device_id=z_mate,
            device_id_type=MESH,
        )

    fetches[0].wait()
    pl.semaphore_wait(barrier, 21)
    for q in range(4):
        map_copy(q).start()

    @pl.loop(0, 8)
    def _(k):
        mate_copy(order(k)).start()

    for fetch in fetches[1:]:
        fetch.wait()
    ws[:, 0:128] = steer[0]
    ws[:, 128:256] = steer[1]

    def weight(level, u, h):
        rows = pl.ds(pl.multiple_of(u * 128, 128), 128)
        cols = pl.ds(pl.multiple_of(h * 128, 128), 128)
        return re_ref[level, rows, cols], im_ref[level, rows, cols]

    for h in range(2):
        c = h * 256
        for side, u in ((0, core), (1, other)):
            r = side * 256
            a, b = weight(0, u, h)
            w0[r : r + 128, c : c + 128] = a
            w0[r : r + 128, c + 128 : c + 256] = b
            w0[r + 128 : r + 256, c : c + 128] = -b
            w0[r + 128 : r + 256, c + 128 : c + 256] = a
        a, b = weight(1, y_hi, h)
        w1[0:128, c : c + 128] = a
        w1[0:128, c + 128 : c + 256] = b
        w1[128:256, c : c + 128] = -b
        w1[128:256, c + 128 : c + 256] = a
    for i, h in ((0, z_lo), (1, 1 - z_lo)):
        a, b = weight(2, z_lo, h)
        c = i * 256
        w2[0:128, c : c + 128] = a
        w2[0:128, c + 128 : c + 256] = -b
        w2[128:256, c : c + 128] = b
        w2[128:256, c + 128 : c + 256] = a

    def chunk(k):
        g = order(k)
        first = jnp.logical_and(g == 0, core == 0)
        last = jnp.logical_and(g == 7, core == 1)
        keep_top = jnp.where(first, 0.0, 1.0).astype(F32)
        keep_bottom = jnp.where(last, 0.0, 1.0).astype(F32)
        own_copy(g).wait()
        drain(pbuf.at[1, g, 64:704], pr.at[g])
        for side in range(2):
            product = dot(pbuf[side, g, 64:704], ws[...])
            qbuf[side, 0], qbuf[side, 1] = product[:, 0:128], product[:, 128:256]
        for side in range(2):
            even, odd = pl.ds(0, 320, stride=2), pl.ds(1, 320, stride=2)
            c = side * 256
            buf0[:, c : c + 128] = (qbuf[side, 0, even, :] - qbuf[side, 1, odd, :]).astype(BF16).astype(F32)
            buf0[:, c + 128 : c + 256] = (qbuf[side, 1, even, :] + qbuf[side, 0, odd, :]).astype(BF16).astype(F32)
        parts = []
        for side, u in ((0, core), (1, other)):
            table = table_ref[0, pl.ds(u, 1), :]
            for part in range(2):
                c = side * 256 + part * 128
                parts.append(shifted(buf0[8:312, c : c + 128], table).astype(BF16))
        merged = dot(jnp.concatenate(parts, axis=1), w0[...]).astype(BF16)
        buf1[0:16, :] = merged[0:16].astype(F32) * keep_top
        buf1[16:272, :] = merged[16:272].astype(F32)
        buf1[272:288, :] = merged[272:288].astype(F32) * keep_bottom
        table = table_ref[1, pl.ds(y_hi, 1), :]
        for s in range(2):
            parts = [shifted(buf1[:, s * 256 + 128 * i : s * 256 + 128 * i + 128], table).astype(BF16) for i in range(2)]
            merged = dot(jnp.concatenate(parts, axis=1), w1[...]).astype(BF16)
            cols = slice(s * 512, s * 512 + 512)
            buf2[0:8, cols] = merged[0:8].astype(F32) * keep_top
            buf2[8:264, cols] = merged[8:264].astype(F32)
            buf2[264:272, cols] = merged[264:272].astype(F32) * keep_bottom
        table = table_ref[2, pl.ds(z_lo, 1), :]
        for i in range(8):
            moved = shifted(buf2[:, 128 * i : 128 * i + 128], table).astype(BF16)
            lhs[g // 4, g % 4, :, :, :, 128 * i : 128 * i + 128] = moved.reshape(4, 2, 32, 128)

    def chunks(start, stop):
        pl.loop(start, stop)(chunk)

    mine = 2 * core + y_hi

    def near_copy(q, kind):
        index = mine if kind < 2 else 2 * core + 1 - y_hi
        return pltpu.make_async_remote_copy(
            src_ref=nbuf.at[q, index],
            dst_ref=nbuf.at[q, index],
            send_sem=ns.at[0],
            recv_sem=nr.at[q, 0 if kind == 0 else 1],
            device_id=y_mate if kind == 0 else core_mate,
            device_id_type=MESH,
        )

    def fold_maps(q):
        map_copy(q).wait_recv()
        cols = slice(q * 128, q * 128 + 128)
        nbuf[q, mine] = (dot(w2[:, 0:256], own_map[:, cols]) + dot(w2[:, 256:512], mbuf[q])).astype(BF16)
        near_copy(q, 0).start()
        near_copy(q, 1).start()

    def forward_maps(q):
        near_copy(q, 0).wait_recv()
        near_copy(q, 2).start()

    def build_maps(q):
        drain(nbuf.at[q, 0:2], nr.at[q, 1])
        for t in range(4):
            re, im = nbuf[q, t, 0:128], nbuf[q, t, 128:256]
            rhs[q, t * 256 : t * 256 + 128, 0:128] = re
            rhs[q, t * 256 : t * 256 + 128, 128:256] = im
            rhs[q, t * 256 + 128 : t * 256 + 256, 0:128] = -im
            rhs[q, t * 256 + 128 : t * 256 + 256, 128:256] = re

    def image_block(n, dest):
        rows = lhs[:, dest] if STREAMS[n] == "x" else lhs[dest % 2, :, :, dest // 2]
        return dot(rows.reshape(512, 1024), rhs[n])

    def first(n):
        return (x, along_x) if STREAMS[n] == "x" else (y, along_y)

    LANES = (slice(0, 128), slice(128, 256))

    def ring_copy(n, slot, part):
        _, to = first(n)
        src, dst = (s1.at[n, slot], r1.at[n, slot]) if part is None else (s1.at[n, slot, part], r1.at[n, slot, part])
        return pltpu.make_async_remote_copy(
            src_ref=src,
            dst_ref=dst,
            send_sem=ss1.at[n],
            recv_sem=rs1.at[n, slot if slot < 2 else 3 if part == 1 else 2],
            device_id=to(TOWARD[slot]),
            device_id_type=MESH,
        )

    def parts_of(n):
        return (None,) if n < 2 else (0, 1)

    def send_far(n):
        here, _ = first(n)
        block = image_block(n, (here + 2) % 4).astype(BF16)
        for h in range(2):
            for part in range(2):
                s1[n, h, part] = block[256 * h : 256 * h + 256, LANES[part]]
            ring_copy(n, h, None).start()

    def send_near(n):
        here, _ = first(n)
        for slot, ahead, h in ((2, 1, 1), (3, 3, 0)):
            block = image_block(n, (here + ahead) % 4)
            mine = block[256 * h : 256 * h + 256].astype(BF16)
            for part in range(2):
                s1[n, slot, part] = mine[:, LANES[part]]
            for part in parts_of(n):
                ring_copy(n, slot, part).start()
            held[n, slot - 2] = block[256 - 256 * h : 512 - 256 * h]

    def take_own(n):
        here, _ = first(n)
        total[n] = image_block(n, here).reshape(2, 2, 2, 2, 32, WIDTH)

    def relay(n):
        for part in parts_of(n):
            for slot in (4, 5):
                if part != 1:
                    ring_copy(n, slot - 4, None).wait_recv()
                for p in (0, 1) if part is None else (part,):
                    value = held[n, slot - 4, :, LANES[p]] + r1[n, slot - 4, p].astype(F32)
                    s1[n, slot, p] = value.astype(BF16)
                ring_copy(n, slot, part).start()

    def gather(n, part):
        if part is None:
            drain(r1.at[n, 2:6], rs1.at[n, 2])
        else:
            drain(r1.at[n, 2:6, part], rs1.at[n, 2 + part])
        for p in (0, 1) if part is None else (part,):
            for h, slots in ((0, (3, 4)), (1, (2, 5))):
                value = total[n, h, :, :, :, :, LANES[p]].reshape(256, 128)
                for slot in slots:
                    value = value + r1[n, slot, p].astype(F32)
                total[n, h, :, :, :, :, LANES[p]] = value.reshape(2, 2, 2, 32, 128)

    def second(n):
        return (y, along_y) if STREAMS[n] == "x" else (x, along_x)

    def straight_copy(n, part, step):
        _, to = second(n)
        src, dst = (sb2.at[n, step - 1], rb2.at[n, step - 1]) if part is None else (
            sa2.at[n - 2, part, step - 1],
            ra2.at[n - 2, part, step - 1],
        )
        return pltpu.make_async_remote_copy(
            src_ref=src,
            dst_ref=dst,
            send_sem=ss2.at[n],
            recv_sem=rs2.at[n, part or 0],
            device_id=to(step),
            device_id_type=MESH,
        )

    def z_copy(n, part, to, its_core, at):
        src, dst = (sb3.at[n, at], rb3.at[n, z]) if part is None else (sa3.at[n - 2, 8 * part + at], ra3.at[n - 2, part, z])
        return pltpu.make_async_remote_copy(
            src_ref=src,
            dst_ref=dst,
            send_sem=ss3.at[n],
            recv_sem=rs3.at[n, part or 0],
            device_id=along_z(to, its_core),
            device_id_type=MESH,
        )

    keeps = core == z // 4

    def start_z(n, part):
        for i in range(4):
            for c in range(2):
                to = 4 * core + i

                @pl.when(z_other(to, c))
                def _():
                    z_copy(n, part, to, c, 2 * i + c).start()

                @pl.when(jnp.logical_not(z_other(to, c)))
                def _():
                    if part is None:
                        rb3[n, z] = sb3[n, 2 * i + c]
                    else:
                        ra3[n - 2, part, z] = sa3[n - 2, 8 * part + 2 * i + c]

    def await_z(n, part):
        got, sem = (rb3.at[n], rs3.at[n, 0]) if part is None else (ra3.at[n - 2, part], rs3.at[n, part])
        pl.when(keeps)(lambda: drain(got.at[0:7], sem))
        pl.when(jnp.logical_not(keeps))(lambda: drain(got, sem))

    def total_block(n, dest, part):
        lanes = LANES[part]
        if STREAMS[n] == "x":
            return total[n, dest % 2, :, :, dest // 2, :, lanes].reshape(128, 128)
        return total[n, dest // 2, dest % 2, :, :, :, lanes].reshape(128, 128)

    def send_straight(n, part):
        gather(n, part)
        here, _ = second(n)
        for step in (2, 1, 3):
            sa2[n - 2, part, step - 1] = total_block(n, (here + step) % 4, part).astype(BF16)
            straight_copy(n, part, step).start()

    def send_z(n, part):
        here, _ = second(n)
        value = total_block(n, here, part)
        drain(ra2.at[n - 2, part], rs2.at[n, part])
        for step in range(3):
            value = value + ra2[n - 2, part, step].astype(F32)
        sa3[n - 2, 8 * part : 8 * part + 8] = value.astype(BF16).reshape(8, 16, 128)
        start_z(n, part)

    def finish(n, part):
        await_z(n, part)
        value = jnp.zeros((16, 128), F32)
        for src in range(8):
            value = value + ra3[n - 2, part, src].astype(F32)
        out_ref[:, part * 512 + n * 128 : part * 512 + n * 128 + 128] = value

    def send_z_early(n):
        gather(n, None)
        for i in range(4):
            for c in range(2):
                rows = slice(16 * c, 16 * c + 16)
                for place in range(4):
                    if STREAMS[n] == "x":
                        block = total[n, place % 2, i // 2, i % 2, place // 2, rows]
                    else:
                        block = total[n, place // 2, place % 2, i // 2, i % 2, rows]
                    sb3[n, 2 * i + c, place] = block.astype(BF16)
        start_z(n, None)

    def send_straight_late(n):
        await_z(n, None)
        value = jnp.zeros((4, 16, WIDTH), F32)
        for src in range(8):
            value = value + rb3[n, src].astype(F32)
        small[n] = value
        here, _ = second(n)
        for step in (2, 1, 3):
            sb2[n, step - 1] = small[n, (here + step) % 4].astype(BF16)
            straight_copy(n, None, step).start()

    def finish_late(n):
        here, _ = second(n)
        value = small[n, here]
        drain(rb2.at[n], rs2.at[n, 0])
        for step in range(3):
            value = value + rb2[n, step].astype(F32)
        for part in range(2):
            out_ref[:, part * 512 + n * 128 : part * 512 + n * 128 + 128] = value[:, LANES[part]]

    def sent_z(n):
        full, some = (sb3.at[n], sb3.at[n, 0:7]) if n < 2 else (sa3.at[n - 2], sa3.at[n - 2, 0:14])
        pl.when(keeps)(lambda: drain(some, ss3.at[n]))
        pl.when(jnp.logical_not(keeps))(lambda: drain(full, ss3.at[n]))

    chunks(0, 3)
    fold_maps(0)
    chunks(3, 4)
    fold_maps(1)
    chunks(4, 6)
    fold_maps(2)
    chunks(6, 7)
    fold_maps(3)
    forward_maps(0)
    chunks(7, 8)
    build_maps(0)
    send_far(0)
    forward_maps(1)
    build_maps(1)
    send_far(1)
    send_near(0)
    forward_maps(2)
    send_near(1)
    forward_maps(3)
    build_maps(2)
    take_own(0)
    take_own(1)
    build_maps(3)
    relay(0)
    relay(1)
    send_far(2)
    send_far(3)
    send_near(2)
    send_z_early(0)
    send_near(3)
    send_z_early(1)
    take_own(2)
    take_own(3)
    relay(2)
    relay(3)
    drain(pulses.at[0:5120], ps.at[0])
    drain(own_map, ms.at[0])
    drain(nbuf.at[:, 0:3], ns.at[0])
    for n in range(2):
        drain(s1.at[n], ss1.at[n])
    send_straight(2, 0)
    send_straight(3, 0)
    send_straight(2, 1)
    send_straight(3, 1)
    send_straight_late(0)
    send_straight_late(1)
    send_z(2, 0)
    send_z(3, 0)
    send_z(2, 1)
    send_z(3, 1)
    finish_late(0)
    finish_late(1)
    for n in range(2):
        drain(s1.at[n + 2], ss1.at[n + 2])
        drain(sb2.at[n], ss2.at[n])
        drain(sa2.at[n], ss2.at[n + 2])
        sent_z(n)
    finish(2, 0)
    finish(3, 0)
    finish(2, 1)
    finish(3, 1)
    sent_z(2)
    sent_z(3)


def body(pulses, steering, merge_re, merge_im, range_shift, image_map):
    vmem = pl.BlockSpec(memory_space=pltpu.VMEM)
    dma = pltpu.SemaphoreType.DMA
    return pl.pallas_call(
        kernel,
        out_shape=jax.ShapeDtypeStruct((16, 1024), F32),
        in_specs=[pl.BlockSpec(memory_space=pltpu.HBM)] * 6,
        out_specs=vmem,
        scratch_shapes=[
            pltpu.VMEM((2, 128, 128), BF16),
            pltpu.VMEM((3, 256, 256), BF16),
            pltpu.VMEM((3, 256, 256), BF16),
            pltpu.VMEM((3, 2, 128), jnp.int32),
            pltpu.VMEM((256, 512), BF16),
            pltpu.VMEM((2, 8, 768, 128), BF16),
            pltpu.VMEM((128, 256), BF16),
            pltpu.VMEM((512, 512), BF16),
            pltpu.VMEM((256, 512), BF16),
            pltpu.VMEM((256, 512), BF16),
            pltpu.VMEM((2, 2, 640, 128), F32),
            pltpu.VMEM((320, 512), F32),
            pltpu.VMEM((288, 512), F32),
            pltpu.VMEM((272, 1024), F32),
            pltpu.VMEM((2, 4, 4, 2, 32, 1024), BF16),
            pltpu.VMEM((4, 256, 128), BF16),
            pltpu.VMEM((4, 4, 256, 128), BF16),
            pltpu.VMEM((4, 1024, WIDTH), BF16),
            pltpu.VMEM((4, 2, 256, WIDTH), F32),
            pltpu.VMEM((4, 2, 2, 2, 2, 32, WIDTH), F32),
            pltpu.VMEM((4, 6, 2, 256, 128), BF16),
            pltpu.VMEM((4, 6, 2, 256, 128), BF16),
            pltpu.VMEM((2, 2, 3, 128, 128), BF16),
            pltpu.VMEM((2, 2, 3, 128, 128), BF16),
            pltpu.VMEM((2, 3, 16, WIDTH), BF16),
            pltpu.VMEM((2, 3, 16, WIDTH), BF16),
            pltpu.VMEM((2, 16, 16, 128), BF16),
            pltpu.VMEM((2, 2, 8, 16, 128), BF16),
            pltpu.VMEM((2, 8, 4, 16, WIDTH), BF16),
            pltpu.VMEM((2, 8, 4, 16, WIDTH), BF16),
            pltpu.VMEM((2, 4, 16, WIDTH), F32),
            dma((5,)),
            dma((8,)),
            dma((1,)),
            dma((8,)),
            dma((1,)),
            dma((4,)),
            dma((1,)),
            dma((4, 2)),
            dma((4,)),
            dma((4, 4)),
            dma((4,)),
            dma((4, 2)),
            dma((4,)),
            dma((4, 2)),
        ],
        compiler_params=pltpu.CompilerParams(
            collective_id=0, has_side_effects=True, vmem_limit_bytes=66_000_000
        ),
        cost_estimate=pl.CostEstimate(flops=8_000_000_000, bytes_accessed=6_000_000, transcendentals=0),
        name="window",
    )(
        pulses.reshape(-1, pulses.shape[2]),
        steering,
        merge_re,
        merge_im,
        range_shift,
        image_map.reshape(256, 512),
    )


def solution(mesh):
    placed = (
        P(None, None, ("pulse", "tile")),
        P(),
        P(),
        P(),
        P(),
        P("pulse", "tile", None, None, None),
    )
    return jax.shard_map(
        body, mesh=mesh, in_specs=placed, out_specs=P(("pulse", "tile"), None), check_vma=False
    )
```

```python
import jax
import jax.numpy as jnp
from jax import lax
from jax.experimental import pallas as pl
from jax.experimental.pallas import tpu as pltpu
from jax.sharding import PartitionSpec as P

MESH = pl.DeviceIdType.MESH
F32 = jnp.float32
BF16 = jnp.bfloat16
WIDTH = 256
STREAMS = ("x", "y", "x", "y")
TOWARD = (1, 3, 1, 3, 1, 3)
Z_FIRST = ((0, 0), (0, 1), (1, 0), (1, 1))


def dot(a, b):
    return jnp.dot(a, b, preferred_element_type=F32)


def shifted(rows, table):
    groups = rows.shape[0] // 8
    at = lax.broadcasted_iota(jnp.int32, (8, 128), 0) + table
    index = jnp.bitwise_and(at + 8, 7)
    below, above = at < 0, at > 7
    picked = [
        jnp.take_along_axis(rows[8 * g : 8 * g + 8], index, axis=0, mode="promise_in_bounds")
        for g in range(groups)
    ]
    return jnp.concatenate(
        [
            jnp.where(below, picked[g - 1], jnp.where(above, picked[g + 1], picked[g]))
            for g in range(1, groups - 1)
        ],
        axis=0,
    )


def kernel(
    pulses, steer_in, re_in, im_in, table_in, map_in, out_ref,
    steer, re_ref, im_ref, table_ref, own_map, pbuf, ws, w0, w1, w2, qbuf, buf0, buf1, buf2, lhs, mbuf, mfar, nbuf, rhs, held, total,
    s1, r1, sa2, ra2, sb2, rb2, sa3, ra3, sb3, rb3, small,
    ins, po, ps, pr, ms, mr, ns, nr, ss1, rs1, ss2, rs2, ss3, rs3, chain,
):
    pulse, tile = lax.axis_index("pulse"), lax.axis_index("tile")
    y_lo, x = pulse // 4, pulse % 4
    z, y_hi, core = tile // 4, (tile // 2) % 2, tile % 2
    y, z_lo, other = 2 * y_hi + y_lo, z % 2, 1 - core

    def along_x(step):
        return (4 * y_lo + (x + step) % 4, tile)

    def along_y(step):
        to = (y + step) % 4
        return (4 * (to % 2) + x, 4 * z + 2 * (to // 2) + core)

    def along_z(to, its_core):
        return (pulse, 4 * to + 2 * y_hi + its_core)

    def z_other(to, its_core):
        return jnp.logical_or(to != z, its_core != core)

    z_mate = along_z(z + 1 - 2 * z_lo, core)
    core_mate = along_z(z, other)
    y_mate = along_y(2)

    fetches = [
        pltpu.make_async_copy(src, dst, ins.at[i])
        for i, (src, dst) in enumerate(
            ((map_in, own_map), (steer_in, steer), (re_in, re_ref), (im_in, im_ref), (table_in, table_ref))
        )
    ]
    for fetch in fetches:
        fetch.start()

    barrier = pltpu.get_barrier_semaphore()
    for step in (1, 2, 3):
        pl.semaphore_signal(barrier, inc=1, device_id=along_x(step), device_id_type=MESH)
        pl.semaphore_signal(barrier, inc=1, device_id=along_y(step), device_id_type=MESH)
    corner = (y_mate[0], 4 * (z + 1 - 2 * z_lo) + 2 * (1 - y_hi) + core)
    near = (core_mate, corner, along_z((z + 1) % 8, core), along_z((z + 7) % 8, core))
    for mate in near:
        pl.semaphore_signal(barrier, inc=1, device_id=mate, device_id_type=MESH)

    def widen(k):
        if k:
            pl.semaphore_wait(chain.at[k - 1], 2)
        for step in (1, 7):
            pl.semaphore_signal(chain.at[k], inc=1, device_id=along_z((z + step) % 8, core), device_id_type=MESH)

    def share_reach():
        pl.semaphore_wait(chain.at[2], 2)
        pl.semaphore_signal(chain.at[3], inc=1, device_id=core_mate, device_id_type=MESH)

    def rows_of(side, g, c):
        wanted = g * 1024 + c * 512 - 64
        start = jnp.clip(wanted, 0, pulses.shape[0] - 640)
        at = 64 + start - wanted
        return (
            pulses.at[pl.ds(pl.multiple_of(start, 64), 640)],
            pbuf.at[side, g, pl.ds(pl.multiple_of(at, 64), 640)],
        )

    def own_copy(g):
        src, dst = rows_of(0, g, core)
        return pltpu.make_async_copy(src, dst, po.at[g])

    def mate_copy(g):
        src, dst = rows_of(1, g, other)
        return pltpu.make_async_remote_copy(
            src_ref=src, dst_ref=dst, send_sem=ps.at[0], recv_sem=pr.at[g], device_id=core_mate, device_id_type=MESH
        )

    def drain(ref, sem):
        pltpu.make_async_copy(ref, ref, sem).wait()

    def order(k):
        ahead = jnp.where(k < 2, 2, jnp.where(k < 4, 1, jnp.where(k < 6, 3, 0)))
        return 4 * (k % 2) + (x + ahead) % 4

    @pl.loop(0, 8)
    def _(k):
        own_copy(order(k)).start()

    zeros = jnp.zeros((64, 128), BF16)

    @pl.when(core == 0)
    def _():
        pbuf[0, 0, 64:128] = zeros
        pbuf[1, 0, 64:128] = zeros

    @pl.when(core == 1)
    def _():
        pbuf[0, 7, 640:704] = zeros
        pbuf[1, 7, 640:704] = zeros

    def map_copy(q, kind):
        return pltpu.make_async_remote_copy(
            src_ref=own_map.at[:, q * 128 : q * 128 + 128],
            dst_ref=mbuf.at[q] if kind == 0 else mfar.at[q, kind - 1],
            send_sem=ms.at[0 if kind == 0 else 1],
            recv_sem=mr.at[q, kind],
            device_id=(z_mate, y_mate, corner)[kind],
            device_id_type=MESH,
        )

    fetches[0].wait()
    pl.semaphore_wait(barrier, 10)
    widen(0)
    for q in range(2):
        for kind in (2, 1, 0):
            map_copy(q, kind).start()
    for q in range(2, 4):
        map_copy(q, 0).start()

    @pl.loop(0, 8)
    def _(k):
        mate_copy(order(k)).start()

    for fetch in fetches[1:]:
        fetch.wait()
    ws[:, 0:128] = steer[0]
    ws[:, 128:256] = steer[1]

    def weight(level, u, h):
        rows = pl.ds(pl.multiple_of(u * 128, 128), 128)
        cols = pl.ds(pl.multiple_of(h * 128, 128), 128)
        return re_ref[level, rows, cols], im_ref[level, rows, cols]

    for h in range(2):
        c = h * 256
        for side, u in ((0, core), (1, other)):
            r = side * 256
            a, b = weight(0, u, h)
            w0[r : r + 128, c : c + 128] = a
            w0[r : r + 128, c + 128 : c + 256] = b
            w0[r + 128 : r + 256, c : c + 128] = -b
            w0[r + 128 : r + 256, c + 128 : c + 256] = a
        a, b = weight(1, y_hi, h)
        w1[0:128, c : c + 128] = a
        w1[0:128, c + 128 : c + 256] = b
        w1[128:256, c : c + 128] = -b
        w1[128:256, c + 128 : c + 256] = a
    for i, h in ((0, z_lo), (1, 1 - z_lo)):
        a, b = weight(2, z_lo, h)
        c = i * 256
        w2[0:128, c : c + 128] = a
        w2[0:128, c + 128 : c + 256] = -b
        w2[128:256, c : c + 128] = b
        w2[128:256, c + 128 : c + 256] = a

    def chunk(k):
        g = order(k)
        first = jnp.logical_and(g == 0, core == 0)
        last = jnp.logical_and(g == 7, core == 1)
        keep_top = jnp.where(first, 0.0, 1.0).astype(F32)
        keep_bottom = jnp.where(last, 0.0, 1.0).astype(F32)
        own_copy(g).wait()
        drain(pbuf.at[1, g, 64:704], pr.at[g])
        for side in range(2):
            product = dot(pbuf[side, g, 64:704], ws[...])
            qbuf[side, 0], qbuf[side, 1] = product[:, 0:128], product[:, 128:256]
        for side in range(2):
            even, odd = pl.ds(0, 320, stride=2), pl.ds(1, 320, stride=2)
            c = side * 256
            buf0[:, c : c + 128] = (qbuf[side, 0, even, :] - qbuf[side, 1, odd, :]).astype(BF16).astype(F32)
            buf0[:, c + 128 : c + 256] = (qbuf[side, 1, even, :] + qbuf[side, 0, odd, :]).astype(BF16).astype(F32)
        parts = []
        for side, u in ((0, core), (1, other)):
            table = table_ref[0, pl.ds(u, 1), :]
            for part in range(2):
                c = side * 256 + part * 128
                parts.append(shifted(buf0[8:312, c : c + 128], table).astype(BF16))
        merged = dot(jnp.concatenate(parts, axis=1), w0[...]).astype(BF16)
        buf1[0:16, :] = merged[0:16].astype(F32) * keep_top
        buf1[16:272, :] = merged[16:272].astype(F32)
        buf1[272:288, :] = merged[272:288].astype(F32) * keep_bottom
        table = table_ref[1, pl.ds(y_hi, 1), :]
        for s in range(2):
            parts = [shifted(buf1[:, s * 256 + 128 * i : s * 256 + 128 * i + 128], table).astype(BF16) for i in range(2)]
            merged = dot(jnp.concatenate(parts, axis=1), w1[...]).astype(BF16)
            cols = slice(s * 512, s * 512 + 512)
            buf2[0:8, cols] = merged[0:8].astype(F32) * keep_top
            buf2[8:264, cols] = merged[8:264].astype(F32)
            buf2[264:272, cols] = merged[264:272].astype(F32) * keep_bottom
        table = table_ref[2, pl.ds(z_lo, 1), :]
        for i in range(8):
            moved = shifted(buf2[:, 128 * i : 128 * i + 128], table).astype(BF16)
            lhs[g // 4, g % 4, :, :, :, 128 * i : 128 * i + 128] = moved.reshape(4, 2, 32, 128)

    def chunks(start, stop):
        pl.loop(start, stop)(chunk)

    mine = 2 * core + y_hi

    def near_copy(q, kind):
        index = mine if kind < 2 else 2 * core + 1 - y_hi
        return pltpu.make_async_remote_copy(
            src_ref=nbuf.at[q, index],
            dst_ref=nbuf.at[q, index],
            send_sem=ns.at[q // 2],
            recv_sem=nr.at[q, 0 if kind == 0 else 1],
            device_id=y_mate if kind == 0 else core_mate,
            device_id_type=MESH,
        )

    def fold_maps(q):
        cols = slice(q * 128, q * 128 + 128)
        for kind in range(3 if q < 2 else 1):
            map_copy(q, kind).wait_recv()
        nbuf[q, mine] = (dot(w2[:, 0:256], own_map[:, cols]) + dot(w2[:, 256:512], mbuf[q])).astype(BF16)
        if q < 2:
            there = dot(w2[:, 0:256], mfar[q, 0]) + dot(w2[:, 256:512], mfar[q, 1])
            nbuf[q, 2 * core + 1 - y_hi] = there.astype(BF16)
            near_copy(q, 2).start()
        else:
            near_copy(q, 0).start()
        near_copy(q, 1).start()

    def forward_maps(q):
        near_copy(q, 0).wait_recv()
        near_copy(q, 2).start()

    def build_maps(q):
        drain(nbuf.at[q, 0:2], nr.at[q, 1])
        for t in range(4):
            re, im = nbuf[q, t, 0:128], nbuf[q, t, 128:256]
            rhs[q, t * 256 : t * 256 + 128, 0:128] = re
            rhs[q, t * 256 : t * 256 + 128, 128:256] = im
            rhs[q, t * 256 + 128 : t * 256 + 256, 0:128] = -im
            rhs[q, t * 256 + 128 : t * 256 + 256, 128:256] = re

    def image_block(n, dest):
        rows = lhs[:, dest] if STREAMS[n] == "x" else lhs[dest % 2, :, :, dest // 2]
        return dot(rows.reshape(512, 1024), rhs[n])

    def first(n):
        return (x, along_x) if STREAMS[n] == "x" else (y, along_y)

    LANES = (slice(0, 128), slice(128, 256))

    LANES = (slice(0, 128), slice(128, 256))

    def ring_copy(n, slot, part):
        _, to = first(n)
        src, dst = (s1.at[n, slot], r1.at[n, slot]) if part is None else (s1.at[n, slot, part], r1.at[n, slot, part])
        return pltpu.make_async_remote_copy(
            src_ref=src,
            dst_ref=dst,
            send_sem=ss1.at[n],
            recv_sem=rs1.at[n, slot if part is None else 2 + part],
            device_id=to(TOWARD[slot]),
            device_id_type=MESH,
        )

    def send_far(n):
        here, _ = first(n)
        block = image_block(n, (here + 2) % 4).astype(BF16)
        for h in range(2):
            for part in range(2):
                s1[n, h, part] = block[256 * h : 256 * h + 256, LANES[part]]
            ring_copy(n, h, None).start()

    def send_near(n):
        here, _ = first(n)
        for slot, ahead, h in ((2, 1, 1), (3, 3, 0)):
            block = image_block(n, (here + ahead) % 4)
            away = block[256 * h : 256 * h + 256].astype(BF16)
            for part in range(2):
                s1[n, slot, part] = away[:, LANES[part]]
                ring_copy(n, slot, part).start()
            held[n, slot - 2] = block[256 - 256 * h : 512 - 256 * h]

    def take_own(n):
        here, _ = first(n)
        total[n] = image_block(n, here).reshape(2, 2, 2, 2, 32, WIDTH)

    def relay(n):
        for part in range(2):
            for slot in (4, 5):
                if part == 0:
                    ring_copy(n, slot - 4, None).wait_recv()
                value = held[n, slot - 4, :, LANES[part]] + r1[n, slot - 4, part].astype(F32)
                s1[n, slot, part] = value.astype(BF16)
                ring_copy(n, slot, part).start()

    def gather(n, part):
        drain(r1.at[n, 2:6, part], rs1.at[n, 2 + part])
        for h, slots in ((0, (3, 4)), (1, (2, 5))):
            value = total[n, h, :, :, :, :, LANES[part]].reshape(256, 128)
            for slot in slots:
                value = value + r1[n, slot, part].astype(F32)
            total[n, h, :, :, :, :, LANES[part]] = value.reshape(2, 2, 2, 32, 128)

    def second(n):
        return (y, along_y) if STREAMS[n] == "x" else (x, along_x)

    def straight_copy(n, part, step):
        _, to = second(n)
        send, recv = (sb2, rb2) if (n, part) in Z_FIRST else (sa2, ra2)
        return pltpu.make_async_remote_copy(
            src_ref=send.at[n, part, step - 1],
            dst_ref=recv.at[n, part, step - 1],
            send_sem=ss2.at[n, part],
            recv_sem=rs2.at[n, part],
            device_id=to(step),
            device_id_type=MESH,
        )

    def z_copy(n, part, to, its_core, at):
        send, recv = (sb3, rb3) if (n, part) in Z_FIRST else (sa3, ra3)
        return pltpu.make_async_remote_copy(
            src_ref=send.at[n, part, at],
            dst_ref=recv.at[n, part, z],
            send_sem=ss3.at[n, part],
            recv_sem=rs3.at[n, part],
            device_id=along_z(to, its_core),
            device_id_type=MESH,
        )

    keeps = core == z // 4

    def start_z(n, part):
        send, recv = (sb3, rb3) if (n, part) in Z_FIRST else (sa3, ra3)
        for i in range(4):
            for c in range(2):
                to, at = 4 * core + i, 2 * i + c

                @pl.when(z_other(to, c))
                def _():
                    z_copy(n, part, to, c, at).start()

                @pl.when(jnp.logical_not(z_other(to, c)))
                def _():
                    recv[n, part, z] = send[n, part, at]

    def drain_z(ref, sem):
        pl.when(keeps)(lambda: drain(ref.at[0:7], sem))
        pl.when(jnp.logical_not(keeps))(lambda: drain(ref, sem))

    def total_block(n, dest, part):
        lanes = LANES[part]
        if STREAMS[n] == "x":
            return total[n, dest % 2, :, :, dest // 2, :, lanes].reshape(128, 128)
        return total[n, dest // 2, dest % 2, :, :, :, lanes].reshape(128, 128)

    def send_straight(n, part):
        gather(n, part)
        here, _ = second(n)
        for step in (2, 1, 3):
            sa2[n, part, step - 1] = total_block(n, (here + step) % 4, part).astype(BF16)
            straight_copy(n, part, step).start()

    def send_z(n, part):
        here, _ = second(n)
        value = total_block(n, here, part)
        drain(ra2.at[n, part], rs2.at[n, part])
        for step in range(3):
            value = value + ra2[n, part, step].astype(F32)
        sa3[n, part] = value.astype(BF16).reshape(8, 16, 128)
        start_z(n, part)

    def send_z_early(n, part):
        gather(n, part)
        lanes = LANES[part]
        for i in range(4):
            for c in range(2):
                rows = slice(16 * c, 16 * c + 16)
                for place in range(4):
                    if STREAMS[n] == "x":
                        block = total[n, place % 2, i // 2, i % 2, place // 2, rows, lanes]
                    else:
                        block = total[n, place // 2, place % 2, i // 2, i % 2, rows, lanes]
                    sb3[n, part, 2 * i + c, place] = block.astype(BF16)
        start_z(n, part)

    def send_straight_late(n, part):
        drain_z(rb3.at[n, part], rs3.at[n, part])
        value = jnp.zeros((4, 16, 128), F32)
        for src in range(8):
            value = value + rb3[n, part, src].astype(F32)
        small[n, part] = value
        here, _ = second(n)
        for step in (2, 1, 3):
            sb2[n, part, step - 1] = small[n, part, (here + step) % 4].astype(BF16)
            straight_copy(n, part, step).start()

    def finish(n, part):
        here, _ = second(n)
        if (n, part) in Z_FIRST:
            value = small[n, part, here]
            drain(rb2.at[n, part], rs2.at[n, part])
            for step in range(3):
                value = value + rb2[n, part, step].astype(F32)
        else:
            drain_z(ra3.at[n, part], rs3.at[n, part])
            value = jnp.zeros((16, 128), F32)
            for src in range(8):
                value = value + ra3[n, part, src].astype(F32)
        out_ref[:, part * 512 + n * 128 : part * 512 + n * 128 + 128] = value

    def sent(n, part):
        if (n, part) in Z_FIRST:
            drain(sb2.at[n, part], ss2.at[n, part])
            drain_z(sb3.at[n, part], ss3.at[n, part])
        else:
            drain(sa2.at[n, part], ss2.at[n, part])
            drain_z(sa3.at[n, part], ss3.at[n, part])

    chunks(0, 5)
    fold_maps(0)
    chunks(5, 7)
    build_maps(0)
    send_far(0)
    fold_maps(1)
    chunks(7, 8)
    build_maps(1)
    fold_maps(2)
    send_far(1)
    widen(1)
    send_near(0)
    fold_maps(3)
    send_near(1)
    widen(2)
    take_own(0)
    relay(0)
    take_own(1)
    forward_maps(2)
    relay(1)
    share_reach()
    build_maps(2)
    send_far(2)
    forward_maps(3)
    build_maps(3)
    send_far(3)
    send_near(2)
    pl.semaphore_wait(chain.at[3], 1)
    send_z_early(0, 0)
    send_z_early(0, 1)
    send_near(3)
    send_z_early(1, 0)
    send_z_early(1, 1)
    take_own(2)
    take_own(3)
    relay(2)
    relay(3)
    drain(pulses.at[0:5120], ps.at[0])
    drain(own_map, ms.at[0])
    drain(own_map, ms.at[1])
    drain(nbuf.at[0:2, 0:2], ns.at[0])
    drain(nbuf.at[2:4, 0:3], ns.at[1])
    for n in range(2):
        drain(s1.at[n], ss1.at[n])
    send_straight(2, 0)
    send_straight(3, 0)
    send_straight(2, 1)
    send_straight(3, 1)
    send_straight_late(0, 0)
    send_straight_late(0, 1)
    send_z(2, 0)
    send_z(3, 0)
    send_straight_late(1, 0)
    send_straight_late(1, 1)
    send_z(2, 1)
    send_z(3, 1)
    for n in range(2):
        drain(s1.at[n + 2], ss1.at[n + 2])
        for part in range(2):
            finish(n, part)
            sent(n, part)
    finish(2, 0)
    finish(3, 0)
    finish(2, 1)
    finish(3, 1)
    for n in range(2, 4):
        for part in range(2):
            sent(n, part)


def body(pulses, steering, merge_re, merge_im, range_shift, image_map):
    vmem = pl.BlockSpec(memory_space=pltpu.VMEM)
    dma = pltpu.SemaphoreType.DMA
    return pl.pallas_call(
        kernel,
        out_shape=pltpu.VMEM((16, 1024), F32),
        in_specs=[pl.BlockSpec(memory_space=pltpu.HBM)] * 6,
        out_specs=vmem,
        scratch_shapes=[
            pltpu.VMEM((2, 128, 128), BF16),
            pltpu.VMEM((3, 256, 256), BF16),
            pltpu.VMEM((3, 256, 256), BF16),
            pltpu.VMEM((3, 2, 128), jnp.int32),
            pltpu.VMEM((256, 512), BF16),
            pltpu.VMEM((2, 8, 768, 128), BF16),
            pltpu.VMEM((128, 256), BF16),
            pltpu.VMEM((512, 512), BF16),
            pltpu.VMEM((256, 512), BF16),
            pltpu.VMEM((256, 512), BF16),
            pltpu.VMEM((2, 2, 640, 128), F32),
            pltpu.VMEM((320, 512), F32),
            pltpu.VMEM((288, 512), F32),
            pltpu.VMEM((272, 1024), F32),
            pltpu.VMEM((2, 4, 4, 2, 32, 1024), BF16),
            pltpu.VMEM((4, 256, 128), BF16),
            pltpu.VMEM((2, 2, 256, 128), BF16),
            pltpu.VMEM((4, 4, 256, 128), BF16),
            pltpu.VMEM((4, 1024, WIDTH), BF16),
            pltpu.VMEM((4, 2, 256, WIDTH), F32),
            pltpu.VMEM((4, 2, 2, 2, 2, 32, WIDTH), F32),
            pltpu.VMEM((4, 6, 2, 256, 128), BF16),
            pltpu.VMEM((4, 6, 2, 256, 128), BF16),
            pltpu.VMEM((4, 2, 3, 128, 128), BF16),
            pltpu.VMEM((4, 2, 3, 128, 128), BF16),
            pltpu.VMEM((4, 2, 3, 16, 128), BF16),
            pltpu.VMEM((4, 2, 3, 16, 128), BF16),
            pltpu.VMEM((4, 2, 8, 16, 128), BF16),
            pltpu.VMEM((4, 2, 8, 16, 128), BF16),
            pltpu.VMEM((4, 2, 8, 4, 16, 128), BF16),
            pltpu.VMEM((4, 2, 8, 4, 16, 128), BF16),
            pltpu.VMEM((4, 2, 4, 16, 128), F32),
            dma((5,)),
            dma((8,)),
            dma((1,)),
            dma((8,)),
            dma((2,)),
            dma((4, 3)),
            dma((2,)),
            dma((4, 2)),
            dma((4,)),
            dma((4, 4)),
            dma((4, 2)),
            dma((4, 2)),
            dma((4, 2)),
            dma((4, 2)),
            pltpu.SemaphoreType.REGULAR((4,)),
        ],
        compiler_params=pltpu.CompilerParams(
            collective_id=0, has_side_effects=True, vmem_limit_bytes=66_000_000
        ),
        cost_estimate=pl.CostEstimate(flops=8_000_000_000, bytes_accessed=6_000_000, transcendentals=0),
        name="window",
    )(
        pulses.reshape(-1, pulses.shape[2]),
        steering,
        merge_re,
        merge_im,
        range_shift,
        image_map.reshape(256, 512),
    )


def solution(mesh):
    placed = (
        P(None, None, ("pulse", "tile")),
        P(),
        P(),
        P(),
        P(),
        P("pulse", "tile", None, None, None),
    )
    return jax.shard_map(
        body, mesh=mesh, in_specs=placed, out_specs=P(("pulse", "tile"), None), check_vma=False
    )
```

```python
import jax
import jax.numpy as jnp
from jax import lax
from jax.experimental import pallas as pl
from jax.experimental.pallas import tpu as pltpu
from jax.sharding import PartitionSpec as P

MESH = pl.DeviceIdType.MESH
F32 = jnp.float32
BF16 = jnp.bfloat16
WIDTH = 256
STREAMS = ("x", "y", "x", "y")
TOWARD = (1, 3, 1, 3, 1, 3)
Z_FIRST = ((0, 0), (0, 1), (1, 0), (1, 1))


def dot(a, b):
    return jnp.dot(a, b, preferred_element_type=F32)


def shifted(rows, table):
    groups = rows.shape[0] // 8
    at = lax.broadcasted_iota(jnp.int32, (8, 128), 0) + table
    index = jnp.bitwise_and(at + 8, 7)
    below, above = at < 0, at > 7
    picked = [
        jnp.take_along_axis(rows[8 * g : 8 * g + 8], index, axis=0, mode="promise_in_bounds")
        for g in range(groups)
    ]
    return jnp.concatenate(
        [
            jnp.where(below, picked[g - 1], jnp.where(above, picked[g + 1], picked[g]))
            for g in range(1, groups - 1)
        ],
        axis=0,
    )


def kernel(
    pulses, steer_in, re_in, im_in, table_in, map_in, out_ref,
    steer, re_ref, im_ref, table_ref, own_map, pbuf, ws, w0, w1, w2, qbuf, buf0, buf1, buf2, lhs, mbuf, mfar, nbuf, rhs, held, total,
    s1, r1, sa2, ra2, sb2, rb2, sa3, ra3, sb3, rb3, small,
    ins, po, ps, pr, ms, mr, ns, nr, ss1, rs1, ss2, rs2, ss3, rs3, chain,
):
    pulse, tile = lax.axis_index("pulse"), lax.axis_index("tile")
    y_lo, x = pulse // 4, pulse % 4
    z, y_hi, core = tile // 4, (tile // 2) % 2, tile % 2
    y, z_lo, other = 2 * y_hi + y_lo, z % 2, 1 - core

    def along_x(step):
        return (4 * y_lo + (x + step) % 4, tile)

    def along_y(step):
        to = (y + step) % 4
        return (4 * (to % 2) + x, 4 * z + 2 * (to // 2) + core)

    def along_z(to, its_core):
        return (pulse, 4 * to + 2 * y_hi + its_core)

    def z_other(to, its_core):
        return jnp.logical_or(to != z, its_core != core)

    z_mate = along_z(z + 1 - 2 * z_lo, core)
    core_mate = along_z(z, other)
    y_mate = along_y(2)

    fetches = [
        pltpu.make_async_copy(src, dst, ins.at[i])
        for i, (src, dst) in enumerate(
            ((map_in, own_map), (steer_in, steer), (re_in, re_ref), (im_in, im_ref), (table_in, table_ref))
        )
    ]
    for fetch in fetches:
        fetch.start()

    barrier = pltpu.get_barrier_semaphore()
    for step in (1, 2, 3):
        pl.semaphore_signal(barrier, inc=1, device_id=along_x(step), device_id_type=MESH)
        pl.semaphore_signal(barrier, inc=1, device_id=along_y(step), device_id_type=MESH)
    corner = (y_mate[0], 4 * (z + 1 - 2 * z_lo) + 2 * (1 - y_hi) + core)
    near = (core_mate, corner, along_z((z + 1) % 8, core), along_z((z + 7) % 8, core))
    for mate in near:
        pl.semaphore_signal(barrier, inc=1, device_id=mate, device_id_type=MESH)

    def widen(k):
        if k:
            pl.semaphore_wait(chain.at[k - 1], 2)
        for step in (1, 7):
            pl.semaphore_signal(chain.at[k], inc=1, device_id=along_z((z + step) % 8, core), device_id_type=MESH)

    def share_reach():
        pl.semaphore_wait(chain.at[2], 2)
        pl.semaphore_signal(chain.at[3], inc=1, device_id=core_mate, device_id_type=MESH)

    def rows_of(side, g, c):
        wanted = g * 1024 + (1 - c) * 512 - 64
        start = jnp.clip(wanted, 0, pulses.shape[0] - 640)
        at = 64 + start - wanted
        return (
            pulses.at[pl.ds(pl.multiple_of(start, 64), 640)],
            pbuf.at[side, g, pl.ds(pl.multiple_of(at, 64), 640)],
        )

    def own_copy(g):
        src, dst = rows_of(0, g, core)
        return pltpu.make_async_copy(src, dst, po.at[g])

    def mate_copy(g):
        src, dst = rows_of(1, g, other)
        return pltpu.make_async_remote_copy(
            src_ref=src, dst_ref=dst, send_sem=ps.at[0], recv_sem=pr.at[g], device_id=core_mate, device_id_type=MESH
        )

    def drain(ref, sem):
        pltpu.make_async_copy(ref, ref, sem).wait()

    def order(k):
        ahead = jnp.where(k < 2, 2, jnp.where(k < 4, 1, jnp.where(k < 6, 3, 0)))
        return 4 * (k % 2) + (x + ahead) % 4

    @pl.loop(0, 8)
    def _(k):
        own_copy(order(k)).start()

    zeros = jnp.zeros((64, 128), BF16)

    @pl.when(core == 1)
    def _():
        pbuf[0, 0, 64:128] = zeros
        pbuf[1, 0, 64:128] = zeros

    @pl.when(core == 0)
    def _():
        pbuf[0, 7, 640:704] = zeros
        pbuf[1, 7, 640:704] = zeros

    def map_copy(q, kind):
        return pltpu.make_async_remote_copy(
            src_ref=own_map.at[:, q * 128 : q * 128 + 128],
            dst_ref=mbuf.at[q] if kind == 0 else mfar.at[q, kind - 1],
            send_sem=ms.at[0 if kind == 0 else 1],
            recv_sem=mr.at[q, kind],
            device_id=(z_mate, y_mate, corner)[kind],
            device_id_type=MESH,
        )

    fetches[0].wait()
    pl.semaphore_wait(barrier, 10)
    widen(0)
    def send_map(q):
        for kind in (2, 1, 0):
            map_copy(q, kind).start()

    send_map(0)

    @pl.loop(0, 8)
    def _(k):
        mate_copy(order(k)).start()

    for fetch in fetches[1:]:
        fetch.wait()
    ws[:, 0:128] = steer[0]
    ws[:, 128:256] = steer[1]

    def weight(level, u, h):
        rows = pl.ds(pl.multiple_of(u * 128, 128), 128)
        cols = pl.ds(pl.multiple_of(h * 128, 128), 128)
        return re_ref[level, rows, cols], im_ref[level, rows, cols]

    for h in range(2):
        c = h * 256
        for side, u in ((0, core), (1, other)):
            r = side * 256
            a, b = weight(0, u, h)
            w0[r : r + 128, c : c + 128] = a
            w0[r : r + 128, c + 128 : c + 256] = b
            w0[r + 128 : r + 256, c : c + 128] = -b
            w0[r + 128 : r + 256, c + 128 : c + 256] = a
        a, b = weight(1, y_hi, h)
        w1[0:128, c : c + 128] = a
        w1[0:128, c + 128 : c + 256] = b
        w1[128:256, c : c + 128] = -b
        w1[128:256, c + 128 : c + 256] = a
    for i, h in ((0, z_lo), (1, 1 - z_lo)):
        a, b = weight(2, z_lo, h)
        c = i * 256
        w2[0:128, c : c + 128] = a
        w2[0:128, c + 128 : c + 256] = -b
        w2[128:256, c : c + 128] = b
        w2[128:256, c + 128 : c + 256] = a

    def chunk(k):
        g = order(k)
        first = jnp.logical_and(g == 0, core == 1)
        last = jnp.logical_and(g == 7, core == 0)
        keep_top = jnp.where(first, 0.0, 1.0).astype(F32)
        keep_bottom = jnp.where(last, 0.0, 1.0).astype(F32)
        own_copy(g).wait()
        drain(pbuf.at[1, g, 64:704], pr.at[g])
        for side in range(2):
            product = dot(pbuf[side, g, 64:704], ws[...])
            qbuf[side, 0], qbuf[side, 1] = product[:, 0:128], product[:, 128:256]
        for side in range(2):
            even, odd = pl.ds(0, 320, stride=2), pl.ds(1, 320, stride=2)
            c = side * 256
            buf0[:, c : c + 128] = (qbuf[side, 0, even, :] - qbuf[side, 1, odd, :]).astype(BF16).astype(F32)
            buf0[:, c + 128 : c + 256] = (qbuf[side, 1, even, :] + qbuf[side, 0, odd, :]).astype(BF16).astype(F32)
        parts = []
        for side, u in ((0, core), (1, other)):
            table = table_ref[0, pl.ds(u, 1), :]
            for part in range(2):
                c = side * 256 + part * 128
                parts.append(shifted(buf0[8:312, c : c + 128], table).astype(BF16))
        merged = dot(jnp.concatenate(parts, axis=1), w0[...]).astype(BF16)
        buf1[0:16, :] = merged[0:16].astype(F32) * keep_top
        buf1[16:272, :] = merged[16:272].astype(F32)
        buf1[272:288, :] = merged[272:288].astype(F32) * keep_bottom
        table = table_ref[1, pl.ds(y_hi, 1), :]
        for s in range(2):
            parts = [shifted(buf1[:, s * 256 + 128 * i : s * 256 + 128 * i + 128], table).astype(BF16) for i in range(2)]
            merged = dot(jnp.concatenate(parts, axis=1), w1[...]).astype(BF16)
            cols = slice(s * 512, s * 512 + 512)
            buf2[0:8, cols] = merged[0:8].astype(F32) * keep_top
            buf2[8:264, cols] = merged[8:264].astype(F32)
            buf2[264:272, cols] = merged[264:272].astype(F32) * keep_bottom
        table = table_ref[2, pl.ds(z_lo, 1), :]
        for i in range(8):
            moved = shifted(buf2[:, 128 * i : 128 * i + 128], table).astype(BF16)
            lhs[g // 4, g % 4, :, :, :, 128 * i : 128 * i + 128] = moved.reshape(4, 2, 32, 128)

    def chunks(start, stop):
        pl.loop(start, stop)(chunk)

    mine = 2 * core + y_hi

    def near_copy(q):
        pair = nbuf.at[q, pl.ds(2 * core, 2)]
        return pltpu.make_async_remote_copy(
            src_ref=pair,
            dst_ref=pair,
            send_sem=ns.at[0],
            recv_sem=nr.at[q],
            device_id=core_mate,
            device_id_type=MESH,
        )

    def fold_maps(q):
        for kind in range(3):
            map_copy(q, kind).wait_recv()
        here = own_map[:, q * 128 : q * 128 + 128], mbuf[q]
        there = mfar[q, 0], mfar[q, 1]
        for index, (a, b) in ((mine, here), (2 * core + 1 - y_hi, there)):
            nbuf[q, index] = (dot(w2[:, 0:256], a) + dot(w2[:, 256:512], b)).astype(BF16)
        near_copy(q).start()

    def build_maps(q):
        near_copy(q).wait_recv()
        for t in range(4):
            re, im = nbuf[q, t, 0:128], nbuf[q, t, 128:256]
            rhs[q, t * 256 : t * 256 + 128, 0:128] = re
            rhs[q, t * 256 : t * 256 + 128, 128:256] = im
            rhs[q, t * 256 + 128 : t * 256 + 256, 0:128] = -im
            rhs[q, t * 256 + 128 : t * 256 + 256, 128:256] = re

    def image_block(n, dest):
        rows = lhs[:, dest] if STREAMS[n] == "x" else lhs[dest % 2, :, :, dest // 2]
        return dot(rows.reshape(512, 1024), rhs[n])

    def first(n):
        return (x, along_x) if STREAMS[n] == "x" else (y, along_y)

    LANES = (slice(0, 128), slice(128, 256))

    LANES = (slice(0, 128), slice(128, 256))

    def ring_copy(n, slot, part):
        _, to = first(n)
        src, dst = (s1.at[n, slot], r1.at[n, slot]) if part is None else (s1.at[n, slot, part], r1.at[n, slot, part])
        return pltpu.make_async_remote_copy(
            src_ref=src,
            dst_ref=dst,
            send_sem=ss1.at[n],
            recv_sem=rs1.at[n, slot if part is None else 2 + part],
            device_id=to(TOWARD[slot]),
            device_id_type=MESH,
        )

    def send_far(n):
        here, _ = first(n)
        block = image_block(n, (here + 2) % 4).astype(BF16)
        for h in range(2):
            for part in range(2):
                s1[n, h, part] = block[256 * h : 256 * h + 256, LANES[part]]
            ring_copy(n, h, None).start()

    def send_near(n):
        here, _ = first(n)
        for slot, ahead, h in ((2, 1, 1), (3, 3, 0)):
            block = image_block(n, (here + ahead) % 4)
            away = block[256 * h : 256 * h + 256].astype(BF16)
            for part in range(2):
                s1[n, slot, part] = away[:, LANES[part]]
                ring_copy(n, slot, part).start()
            held[n, slot - 2] = block[256 - 256 * h : 512 - 256 * h]

    def take_own(n):
        here, _ = first(n)
        total[n] = image_block(n, here).reshape(2, 2, 2, 2, 32, WIDTH)

    def relay(n):
        for part in range(2):
            for slot in (4, 5):
                if part == 0:
                    ring_copy(n, slot - 4, None).wait_recv()
                value = held[n, slot - 4, :, LANES[part]] + r1[n, slot - 4, part].astype(F32)
                s1[n, slot, part] = value.astype(BF16)
                ring_copy(n, slot, part).start()

    def gather(n, part):
        drain(r1.at[n, 2:6, part], rs1.at[n, 2 + part])
        for h, slots in ((0, (3, 4)), (1, (2, 5))):
            value = total[n, h, :, :, :, :, LANES[part]].reshape(256, 128)
            for slot in slots:
                value = value + r1[n, slot, part].astype(F32)
            total[n, h, :, :, :, :, LANES[part]] = value.reshape(2, 2, 2, 32, 128)

    def second(n):
        return (y, along_y) if STREAMS[n] == "x" else (x, along_x)

    def straight_copy(n, part, step):
        _, to = second(n)
        send, recv = (sb2, rb2) if (n, part) in Z_FIRST else (sa2, ra2)
        return pltpu.make_async_remote_copy(
            src_ref=send.at[n, part, step - 1],
            dst_ref=recv.at[n, part, step - 1],
            send_sem=ss2.at[n, part],
            recv_sem=rs2.at[n, part],
            device_id=to(step),
            device_id_type=MESH,
        )

    def z_copy(n, part, to, its_core, at):
        send, recv = (sb3, rb3) if (n, part) in Z_FIRST else (sa3, ra3)
        return pltpu.make_async_remote_copy(
            src_ref=send.at[n, part, at],
            dst_ref=recv.at[n, part, z],
            send_sem=ss3.at[n, part],
            recv_sem=rs3.at[n, part],
            device_id=along_z(to, its_core),
            device_id_type=MESH,
        )

    keeps = core == 1 - z // 4

    def start_z(n, part):
        send, recv = (sb3, rb3) if (n, part) in Z_FIRST else (sa3, ra3)
        for i in range(4):
            for c in range(2):
                to, at = 4 * other + i, 2 * i + c

                @pl.when(z_other(to, c))
                def _():
                    z_copy(n, part, to, c, at).start()

                @pl.when(jnp.logical_not(z_other(to, c)))
                def _():
                    recv[n, part, z] = send[n, part, at]

    def drain_z(ref, sem):
        pl.when(keeps)(lambda: drain(ref.at[0:7], sem))
        pl.when(jnp.logical_not(keeps))(lambda: drain(ref, sem))

    def total_block(n, dest, part):
        lanes = LANES[part]
        if STREAMS[n] == "x":
            return total[n, dest % 2, :, :, dest // 2, :, lanes].reshape(128, 128)
        return total[n, dest // 2, dest % 2, :, :, :, lanes].reshape(128, 128)

    def send_straight(n, part):
        gather(n, part)
        here, _ = second(n)
        for step in (2, 1, 3):
            sa2[n, part, step - 1] = total_block(n, (here + step) % 4, part).astype(BF16)
            straight_copy(n, part, step).start()

    def send_z(n, part):
        here, _ = second(n)
        value = total_block(n, here, part)
        drain(ra2.at[n, part], rs2.at[n, part])
        for step in range(3):
            value = value + ra2[n, part, step].astype(F32)
        sa3[n, part] = value.astype(BF16).reshape(8, 16, 128)
        start_z(n, part)

    def send_z_early(n, part):
        gather(n, part)
        lanes = LANES[part]
        for i in range(4):
            for c in range(2):
                rows = slice(16 * c, 16 * c + 16)
                for place in range(4):
                    if STREAMS[n] == "x":
                        block = total[n, place % 2, i // 2, i % 2, place // 2, rows, lanes]
                    else:
                        block = total[n, place // 2, place % 2, i // 2, i % 2, rows, lanes]
                    sb3[n, part, 2 * i + c, place] = block.astype(BF16)
        start_z(n, part)

    def send_straight_late(n, part):
        drain_z(rb3.at[n, part], rs3.at[n, part])
        value = jnp.zeros((4, 16, 128), F32)
        for src in range(8):
            value = value + rb3[n, part, src].astype(F32)
        small[n, part] = value
        here, _ = second(n)
        for step in (2, 1, 3):
            sb2[n, part, step - 1] = small[n, part, (here + step) % 4].astype(BF16)
            straight_copy(n, part, step).start()

    def finish(n, part):
        here, _ = second(n)
        if (n, part) in Z_FIRST:
            value = small[n, part, here]
            drain(rb2.at[n, part], rs2.at[n, part])
            for step in range(3):
                value = value + rb2[n, part, step].astype(F32)
        else:
            drain_z(ra3.at[n, part], rs3.at[n, part])
            value = jnp.zeros((16, 128), F32)
            for src in range(8):
                value = value + ra3[n, part, src].astype(F32)
        out_ref[:, part * 512 + n * 128 : part * 512 + n * 128 + 128] = value

    def sent(n, part):
        if (n, part) in Z_FIRST:
            drain(sb2.at[n, part], ss2.at[n, part])
            drain_z(sb3.at[n, part], ss3.at[n, part])
        else:
            drain(sa2.at[n, part], ss2.at[n, part])
            drain_z(sa3.at[n, part], ss3.at[n, part])

    chunks(0, 2)
    send_map(1)
    chunks(2, 4)
    send_map(2)
    chunks(4, 5)
    send_map(3)
    fold_maps(0)
    chunks(5, 7)
    build_maps(0)
    send_far(0)
    fold_maps(1)
    chunks(7, 8)
    build_maps(1)
    send_far(1)
    widen(1)
    send_near(0)
    fold_maps(2)
    send_near(1)
    relay(0)
    widen(2)
    build_maps(2)
    send_far(2)
    take_own(0)
    fold_maps(3)
    take_own(1)
    relay(1)
    build_maps(3)
    send_far(3)
    share_reach()
    send_near(2)
    pl.semaphore_wait(chain.at[3], 1)
    send_z_early(0, 0)
    send_z_early(0, 1)
    send_near(3)
    send_z_early(1, 0)
    send_z_early(1, 1)
    take_own(2)
    relay(2)
    take_own(3)
    relay(3)
    drain(pulses.at[0:5120], ps.at[0])
    drain(own_map, ms.at[0])
    drain(mfar, ms.at[1])
    drain(nbuf.at[:, 0:2], ns.at[0])
    for n in range(2):
        drain(s1.at[n], ss1.at[n])
    send_straight(2, 0)
    send_straight(3, 0)
    send_straight(2, 1)
    send_straight(3, 1)
    send_straight_late(0, 0)
    send_straight_late(0, 1)
    send_z(2, 0)
    send_z(3, 0)
    send_straight_late(1, 0)
    send_straight_late(1, 1)
    send_z(2, 1)
    send_z(3, 1)
    for n in range(2):
        drain(s1.at[n + 2], ss1.at[n + 2])
        for part in range(2):
            finish(n, part)
            sent(n, part)
    finish(2, 0)
    finish(3, 0)
    finish(2, 1)
    finish(3, 1)
    for n in range(2, 4):
        for part in range(2):
            sent(n, part)


def body(pulses, steering, merge_re, merge_im, range_shift, image_map):
    vmem = pl.BlockSpec(memory_space=pltpu.VMEM)
    dma = pltpu.SemaphoreType.DMA
    return pl.pallas_call(
        kernel,
        out_shape=pltpu.VMEM((16, 1024), F32),
        in_specs=[pl.BlockSpec(memory_space=pltpu.HBM)] * 6,
        out_specs=vmem,
        scratch_shapes=[
            pltpu.VMEM((2, 128, 128), BF16),
            pltpu.VMEM((3, 256, 256), BF16),
            pltpu.VMEM((3, 256, 256), BF16),
            pltpu.VMEM((3, 2, 128), jnp.int32),
            pltpu.VMEM((256, 512), BF16),
            pltpu.VMEM((2, 8, 768, 128), BF16),
            pltpu.VMEM((128, 256), BF16),
            pltpu.VMEM((512, 512), BF16),
            pltpu.VMEM((256, 512), BF16),
            pltpu.VMEM((256, 512), BF16),
            pltpu.VMEM((2, 2, 640, 128), F32),
            pltpu.VMEM((320, 512), F32),
            pltpu.VMEM((288, 512), F32),
            pltpu.VMEM((272, 1024), F32),
            pltpu.VMEM((2, 4, 4, 2, 32, 1024), BF16),
            pltpu.VMEM((4, 256, 128), BF16),
            pltpu.VMEM((4, 2, 256, 128), BF16),
            pltpu.VMEM((4, 4, 256, 128), BF16),
            pltpu.VMEM((4, 1024, WIDTH), BF16),
            pltpu.VMEM((4, 2, 256, WIDTH), F32),
            pltpu.VMEM((4, 2, 2, 2, 2, 32, WIDTH), F32),
            pltpu.VMEM((4, 6, 2, 256, 128), BF16),
            pltpu.VMEM((4, 6, 2, 256, 128), BF16),
            pltpu.VMEM((4, 2, 3, 128, 128), BF16),
            pltpu.VMEM((4, 2, 3, 128, 128), BF16),
            pltpu.VMEM((4, 2, 3, 16, 128), BF16),
            pltpu.VMEM((4, 2, 3, 16, 128), BF16),
            pltpu.VMEM((4, 2, 8, 16, 128), BF16),
            pltpu.VMEM((4, 2, 8, 16, 128), BF16),
            pltpu.VMEM((4, 2, 8, 4, 16, 128), BF16),
            pltpu.VMEM((4, 2, 8, 4, 16, 128), BF16),
            pltpu.VMEM((4, 2, 4, 16, 128), F32),
            dma((5,)),
            dma((8,)),
            dma((1,)),
            dma((8,)),
            dma((2,)),
            dma((4, 3)),
            dma((1,)),
            dma((4,)),
            dma((4,)),
            dma((4, 4)),
            dma((4, 2)),
            dma((4, 2)),
            dma((4, 2)),
            dma((4, 2)),
            pltpu.SemaphoreType.REGULAR((4,)),
        ],
        compiler_params=pltpu.CompilerParams(
            collective_id=0, has_side_effects=True, vmem_limit_bytes=66_000_000
        ),
        cost_estimate=pl.CostEstimate(flops=8_000_000_000, bytes_accessed=6_000_000, transcendentals=0),
        name="window",
    )(
        pulses.reshape(-1, pulses.shape[2]),
        steering,
        merge_re,
        merge_im,
        range_shift,
        image_map.reshape(256, 512),
    )


def solution(mesh):
    placed = (
        P(None, None, ("pulse", "tile")),
        P(),
        P(),
        P(),
        P(),
        P("pulse", "tile", None, None, None),
    )
    return jax.shard_map(
        body, mesh=mesh, in_specs=placed, out_specs=P(("pulse", "tile"), None), check_vma=False
    )
```

```python
import jax
import jax.numpy as jnp
from jax import lax
from jax.experimental import pallas as pl
from jax.experimental.pallas import tpu as pltpu
from jax.sharding import PartitionSpec as P

MESH = pl.DeviceIdType.MESH
F32 = jnp.float32
BF16 = jnp.bfloat16
WIDTH = 256
STREAMS = ("x", "y", "x", "y")
TOWARD = (1, 3, 1, 3, 1, 3)
Z_FIRST = ((0, 0), (0, 1), (1, 0), (1, 1))


def dot(a, b):
    return jnp.dot(a, b, preferred_element_type=F32)


def shifted(rows, table):
    groups = rows.shape[0] // 8
    at = lax.broadcasted_iota(jnp.int32, (8, 128), 0) + table
    index = jnp.bitwise_and(at + 8, 7)
    below, above = at < 0, at > 7
    picked = [
        jnp.take_along_axis(rows[8 * g : 8 * g + 8], index, axis=0, mode="promise_in_bounds")
        for g in range(groups)
    ]
    return jnp.concatenate(
        [
            jnp.where(below, picked[g - 1], jnp.where(above, picked[g + 1], picked[g]))
            for g in range(1, groups - 1)
        ],
        axis=0,
    )


def kernel(
    pulses, steer_in, re_in, im_in, table_in, map_in, out_ref,
    steer, re_ref, im_ref, table_ref, own_map, pbuf, ws, w0, w1, w2, qbuf, buf0, buf1, buf2, lhs, mbuf, mfar, nbuf, rhs, held, total,
    s1, r1, sa2, ra2, sb2, rb2, sa3, ra3, sb3, rb3, small,
    ins, po, ps, pr, ms, mr, ns, nr, ss1, rs1, ss2, rs2, ss3, rs3, chain,
):
    pulse, tile = lax.axis_index("pulse"), lax.axis_index("tile")
    y_lo, x = pulse // 4, pulse % 4
    z, y_hi, core = tile // 4, (tile // 2) % 2, tile % 2
    y, z_lo, other = 2 * y_hi + y_lo, z % 2, 1 - core

    def along_x(step):
        return (4 * y_lo + (x + step) % 4, tile)

    def along_y(step):
        to = (y + step) % 4
        return (4 * (to % 2) + x, 4 * z + 2 * (to // 2) + core)

    def along_z(to, its_core):
        return (pulse, 4 * to + 2 * y_hi + its_core)

    def z_other(to, its_core):
        return jnp.logical_or(to != z, its_core != core)

    z_mate = along_z(z + 1 - 2 * z_lo, core)
    core_mate = along_z(z, other)
    y_mate = along_y(2)

    fetches = [
        pltpu.make_async_copy(src, dst, ins.at[i])
        for i, (src, dst) in enumerate(
            ((map_in, own_map), (steer_in, steer), (re_in, re_ref), (im_in, im_ref), (table_in, table_ref))
        )
    ]
    for fetch in fetches:
        fetch.start()

    barrier = pltpu.get_barrier_semaphore()
    for step in (1, 2, 3):
        pl.semaphore_signal(barrier, inc=1, device_id=along_x(step), device_id_type=MESH)
        pl.semaphore_signal(barrier, inc=1, device_id=along_y(step), device_id_type=MESH)
    corner = (y_mate[0], 4 * (z + 1 - 2 * z_lo) + 2 * (1 - y_hi) + core)
    near = (core_mate, corner, along_z((z + 1) % 8, core), along_z((z + 7) % 8, core))
    for mate in near:
        pl.semaphore_signal(barrier, inc=1, device_id=mate, device_id_type=MESH)

    def widen(k):
        if k:
            pl.semaphore_wait(chain.at[k - 1], 2)
        for step in (1, 7):
            pl.semaphore_signal(chain.at[k], inc=1, device_id=along_z((z + step) % 8, core), device_id_type=MESH)

    def share_reach():
        pl.semaphore_wait(chain.at[2], 2)
        pl.semaphore_signal(chain.at[3], inc=1, device_id=core_mate, device_id_type=MESH)

    def rows_of(side, g, c):
        wanted = g * 1024 + (1 - c) * 512 - 64
        start = jnp.clip(wanted, 0, pulses.shape[0] - 640)
        at = 64 + start - wanted
        return (
            pulses.at[pl.ds(pl.multiple_of(start, 64), 640)],
            pbuf.at[side, g, pl.ds(pl.multiple_of(at, 64), 640)],
        )

    def own_copy(g):
        src, dst = rows_of(0, g, core)
        return pltpu.make_async_copy(src, dst, po.at[g])

    def mate_copy(g):
        src, dst = rows_of(1, g, other)
        return pltpu.make_async_remote_copy(
            src_ref=src, dst_ref=dst, send_sem=ps.at[0], recv_sem=pr.at[g], device_id=core_mate, device_id_type=MESH
        )

    def drain(ref, sem):
        pltpu.make_async_copy(ref, ref, sem).wait()

    def order(k):
        ahead = jnp.where(k < 2, 2, jnp.where(k < 4, 1, jnp.where(k < 6, 3, 0)))
        return 4 * (k % 2) + (x + ahead) % 4

    @pl.loop(0, 8)
    def _(k):
        own_copy(order(k)).start()

    zeros = jnp.zeros((64, 128), BF16)

    @pl.when(core == 1)
    def _():
        pbuf[0, 0, 64:128] = zeros
        pbuf[1, 0, 64:128] = zeros

    @pl.when(core == 0)
    def _():
        pbuf[0, 7, 640:704] = zeros
        pbuf[1, 7, 640:704] = zeros

    def map_copy(q, kind):
        return pltpu.make_async_remote_copy(
            src_ref=own_map.at[:, q * 128 : q * 128 + 128],
            dst_ref=mbuf.at[q] if kind == 0 else mfar.at[q, kind - 1],
            send_sem=ms.at[0 if kind == 0 else 1],
            recv_sem=mr.at[q, kind],
            device_id=(z_mate, y_mate, corner)[kind],
            device_id_type=MESH,
        )

    fetches[0].wait()
    pl.semaphore_wait(barrier, 10)
    widen(0)
    def send_map(q):
        for kind in (2, 1, 0):
            map_copy(q, kind).start()

    send_map(0)

    @pl.loop(0, 8)
    def _(k):
        mate_copy(order(k)).start()

    for fetch in fetches[1:]:
        fetch.wait()
    ws[:, 0:128] = steer[0]
    ws[:, 128:256] = steer[1]

    def weight(level, u, h):
        rows = pl.ds(pl.multiple_of(u * 128, 128), 128)
        cols = pl.ds(pl.multiple_of(h * 128, 128), 128)
        return re_ref[level, rows, cols], im_ref[level, rows, cols]

    for h in range(2):
        c = h * 256
        for side, u in ((0, core), (1, other)):
            r = side * 256
            a, b = weight(0, u, h)
            w0[r : r + 128, c : c + 128] = a
            w0[r : r + 128, c + 128 : c + 256] = b
            w0[r + 128 : r + 256, c : c + 128] = -b
            w0[r + 128 : r + 256, c + 128 : c + 256] = a
        a, b = weight(1, y_hi, h)
        w1[0:128, c : c + 128] = a
        w1[0:128, c + 128 : c + 256] = b
        w1[128:256, c : c + 128] = -b
        w1[128:256, c + 128 : c + 256] = a
    for i, h in ((0, z_lo), (1, 1 - z_lo)):
        a, b = weight(2, z_lo, h)
        c = i * 256
        w2[0:128, c : c + 128] = a
        w2[0:128, c + 128 : c + 256] = -b
        w2[128:256, c : c + 128] = b
        w2[128:256, c + 128 : c + 256] = a

    def chunk(k):
        g = order(k)
        first = jnp.logical_and(g == 0, core == 1)
        last = jnp.logical_and(g == 7, core == 0)
        keep_top = jnp.where(first, 0.0, 1.0).astype(F32)
        keep_bottom = jnp.where(last, 0.0, 1.0).astype(F32)
        own_copy(g).wait()
        drain(pbuf.at[1, g, 64:704], pr.at[g])
        for side in range(2):
            product = dot(pbuf[side, g, 64:704], ws[...])
            qbuf[side, 0, 0:640], qbuf[side, 1, 0:640] = product[:, 0:128], product[:, 128:256]
        for side in range(2):
            even, odd = pl.ds(0, 320, stride=2), pl.ds(1, 320, stride=2)
            c = side * 256
            buf0[:, c : c + 128] = (qbuf[side, 0, even, :] - qbuf[side, 1, odd, :]).astype(BF16).astype(F32)
            buf0[:, c + 128 : c + 256] = (qbuf[side, 1, even, :] + qbuf[side, 0, odd, :]).astype(BF16).astype(F32)
        parts = []
        for side, u in ((0, core), (1, other)):
            table = table_ref[0, pl.ds(u, 1), :]
            for part in range(2):
                c = side * 256 + part * 128
                parts.append(shifted(buf0[8:312, c : c + 128], table).astype(BF16))
        merged = dot(jnp.concatenate(parts, axis=1), w0[...]).astype(BF16)
        buf1[0:16, :] = merged[0:16].astype(F32) * keep_top
        buf1[16:272, :] = merged[16:272].astype(F32)
        buf1[272:288, :] = merged[272:288].astype(F32) * keep_bottom
        table = table_ref[1, pl.ds(y_hi, 1), :]
        for s in range(2):
            parts = [shifted(buf1[:, s * 256 + 128 * i : s * 256 + 128 * i + 128], table).astype(BF16) for i in range(2)]
            merged = dot(jnp.concatenate(parts, axis=1), w1[...]).astype(BF16)
            cols = slice(s * 512, s * 512 + 512)
            buf2[0:8, cols] = merged[0:8].astype(F32) * keep_top
            buf2[8:264, cols] = merged[8:264].astype(F32)
            buf2[264:272, cols] = merged[264:272].astype(F32) * keep_bottom
        table = table_ref[2, pl.ds(z_lo, 1), :]
        for i in range(8):
            moved = shifted(buf2[:, 128 * i : 128 * i + 128], table).astype(BF16)
            lhs[g // 4, g % 4, :, :, :, 128 * i : 128 * i + 128] = moved.reshape(4, 2, 32, 128)

    def chunks(start, stop):
        pl.loop(start, stop)(chunk)

    mine = 2 * core + y_hi

    def near_copy(q):
        pair = nbuf.at[q, pl.ds(2 * core, 2)]
        return pltpu.make_async_remote_copy(
            src_ref=pair,
            dst_ref=pair,
            send_sem=ns.at[0],
            recv_sem=nr.at[q],
            device_id=core_mate,
            device_id_type=MESH,
        )

    def fold_maps(q):
        for kind in range(3):
            map_copy(q, kind).wait_recv()
        here = own_map[:, q * 128 : q * 128 + 128], mbuf[q]
        there = mfar[q, 0], mfar[q, 1]
        for index, (a, b) in ((mine, here), (2 * core + 1 - y_hi, there)):
            nbuf[q, index] = (dot(w2[:, 0:256], a) + dot(w2[:, 256:512], b)).astype(BF16)
        near_copy(q).start()

    def build_maps(q):
        near_copy(q).wait_recv()
        for t in range(4):
            re, im = nbuf[q, t, 0:128], nbuf[q, t, 128:256]
            rhs[q, t * 256 : t * 256 + 128, 0:128] = re
            rhs[q, t * 256 : t * 256 + 128, 128:256] = im
            rhs[q, t * 256 + 128 : t * 256 + 256, 0:128] = -im
            rhs[q, t * 256 + 128 : t * 256 + 256, 128:256] = re

    def image_block(n, dest):
        rows = lhs[:, dest] if STREAMS[n] == "x" else lhs[dest % 2, :, :, dest // 2]
        return dot(rows.reshape(512, 1024), rhs[n])

    def first(n):
        return (x, along_x) if STREAMS[n] == "x" else (y, along_y)

    LANES = (slice(0, 128), slice(128, 256))

    LANES = (slice(0, 128), slice(128, 256))

    def ring_copy(n, slot, part):
        _, to = first(n)
        src, dst = (s1.at[n, slot], r1.at[n, slot]) if part is None else (s1.at[n, slot, part], r1.at[n, slot, part])
        return pltpu.make_async_remote_copy(
            src_ref=src,
            dst_ref=dst,
            send_sem=ss1.at[n],
            recv_sem=rs1.at[n, slot if part is None else 2 + part],
            device_id=to(TOWARD[slot]),
            device_id_type=MESH,
        )

    def send_far(n):
        here, _ = first(n)
        block = image_block(n, (here + 2) % 4).astype(BF16)
        for h in range(2):
            for part in range(2):
                s1[n, h, part] = block[256 * h : 256 * h + 256, LANES[part]]
            ring_copy(n, h, None).start()

    def send_near(n):
        here, _ = first(n)
        for slot, ahead, h in ((2, 1, 1), (3, 3, 0)):
            block = image_block(n, (here + ahead) % 4)
            away = block[256 * h : 256 * h + 256].astype(BF16)
            for part in range(2):
                s1[n, slot, part] = away[:, LANES[part]]
                ring_copy(n, slot, part).start()
            held[n, slot - 2] = block[256 - 256 * h : 512 - 256 * h]

    def take_own(n):
        here, _ = first(n)
        total[n] = image_block(n, here).reshape(2, 2, 2, 2, 32, WIDTH)

    def relay(n):
        for part in range(2):
            for slot in (4, 5):
                if part == 0:
                    ring_copy(n, slot - 4, None).wait_recv()
                value = held[n, slot - 4, :, LANES[part]] + r1[n, slot - 4, part].astype(F32)
                s1[n, slot, part] = value.astype(BF16)
                ring_copy(n, slot, part).start()

    def gather(n, part):
        drain(r1.at[n, 2:6, part], rs1.at[n, 2 + part])
        for h, slots in ((0, (3, 4)), (1, (2, 5))):
            value = total[n, h, :, :, :, :, LANES[part]].reshape(256, 128)
            for slot in slots:
                value = value + r1[n, slot, part].astype(F32)
            total[n, h, :, :, :, :, LANES[part]] = value.reshape(2, 2, 2, 32, 128)

    def second(n):
        return (y, along_y) if STREAMS[n] == "x" else (x, along_x)

    def straight_copy(n, part, step):
        _, to = second(n)
        send, recv = (sb2, rb2) if (n, part) in Z_FIRST else (sa2, ra2)
        return pltpu.make_async_remote_copy(
            src_ref=send.at[n, part, step - 1],
            dst_ref=recv.at[n, part, step - 1],
            send_sem=ss2.at[n, part],
            recv_sem=rs2.at[n, part],
            device_id=to(step),
            device_id_type=MESH,
        )

    def z_copy(n, part, to, its_core, at):
        send, recv = (sb3, rb3) if (n, part) in Z_FIRST else (sa3, ra3)
        return pltpu.make_async_remote_copy(
            src_ref=send.at[n, part, at],
            dst_ref=recv.at[n, part, z],
            send_sem=ss3.at[n, part],
            recv_sem=rs3.at[n, part],
            device_id=along_z(to, its_core),
            device_id_type=MESH,
        )

    keeps = core == 1 - z // 4

    def start_z(n, part):
        send, recv = (sb3, rb3) if (n, part) in Z_FIRST else (sa3, ra3)
        for i in range(4):
            for c in range(2):
                to, at = 4 * other + i, 2 * i + c

                @pl.when(z_other(to, c))
                def _():
                    z_copy(n, part, to, c, at).start()

                @pl.when(jnp.logical_not(z_other(to, c)))
                def _():
                    recv[n, part, z] = send[n, part, at]

    def drain_z(ref, sem):
        pl.when(keeps)(lambda: drain(ref.at[0:7], sem))
        pl.when(jnp.logical_not(keeps))(lambda: drain(ref, sem))

    def total_block(n, dest, part):
        lanes = LANES[part]
        if STREAMS[n] == "x":
            return total[n, dest % 2, :, :, dest // 2, :, lanes].reshape(128, 128)
        return total[n, dest // 2, dest % 2, :, :, :, lanes].reshape(128, 128)

    def send_straight(n, part):
        gather(n, part)
        here, _ = second(n)
        for step in (2, 1, 3):
            sa2[n, part, step - 1] = total_block(n, (here + step) % 4, part).astype(BF16)
            straight_copy(n, part, step).start()

    def send_z(n, part):
        here, _ = second(n)
        value = total_block(n, here, part)
        drain(ra2.at[n, part], rs2.at[n, part])
        for step in range(3):
            value = value + ra2[n, part, step].astype(F32)
        sa3[n, part] = value.astype(BF16).reshape(8, 16, 128)
        start_z(n, part)

    def send_z_early(n, part):
        gather(n, part)
        lanes = LANES[part]
        for i in range(4):
            for c in range(2):
                rows = slice(16 * c, 16 * c + 16)
                for place in range(4):
                    if STREAMS[n] == "x":
                        block = total[n, place % 2, i // 2, i % 2, place // 2, rows, lanes]
                    else:
                        block = total[n, place // 2, place % 2, i // 2, i % 2, rows, lanes]
                    sb3[n, part, 2 * i + c, place] = block.astype(BF16)
        start_z(n, part)

    def send_straight_late(n, part):
        drain_z(rb3.at[n, part], rs3.at[n, part])
        value = jnp.zeros((4, 16, 128), F32)
        for src in range(8):
            value = value + rb3[n, part, src].astype(F32)
        small[n, part] = value
        here, _ = second(n)
        for step in (2, 1, 3):
            sb2[n, part, step - 1] = small[n, part, (here + step) % 4].astype(BF16)
            straight_copy(n, part, step).start()

    def finish(n, part):
        here, _ = second(n)
        if (n, part) in Z_FIRST:
            value = small[n, part, here]
            drain(rb2.at[n, part], rs2.at[n, part])
            for step in range(3):
                value = value + rb2[n, part, step].astype(F32)
        else:
            drain_z(ra3.at[n, part], rs3.at[n, part])
            value = jnp.zeros((16, 128), F32)
            for src in range(8):
                value = value + ra3[n, part, src].astype(F32)
        out_ref[:, part * 512 + n * 128 : part * 512 + n * 128 + 128] = value

    def sent(n, part):
        if (n, part) in Z_FIRST:
            drain(sb2.at[n, part], ss2.at[n, part])
            drain_z(sb3.at[n, part], ss3.at[n, part])
        else:
            drain(sa2.at[n, part], ss2.at[n, part])
            drain_z(sa3.at[n, part], ss3.at[n, part])

    chunks(0, 2)
    send_map(1)
    chunks(2, 4)
    send_map(2)
    chunks(4, 5)
    send_map(3)
    fold_maps(0)
    chunks(5, 7)
    build_maps(0)
    send_far(0)
    fold_maps(1)
    chunks(7, 8)
    build_maps(1)
    send_far(1)
    widen(1)
    send_near(0)
    fold_maps(2)
    send_near(1)
    relay(0)
    widen(2)
    build_maps(2)
    send_far(2)
    take_own(0)
    fold_maps(3)
    take_own(1)
    relay(1)
    build_maps(3)
    send_far(3)
    share_reach()
    send_near(2)
    pl.semaphore_wait(chain.at[3], 1)
    send_z_early(0, 0)
    send_z_early(0, 1)
    send_near(3)
    send_z_early(1, 0)
    send_z_early(1, 1)
    take_own(2)
    relay(2)
    take_own(3)
    relay(3)
    drain(pulses.at[0:5120], ps.at[0])
    drain(own_map, ms.at[0])
    drain(mfar, ms.at[1])
    drain(nbuf.at[:, 0:2], ns.at[0])
    for n in range(2):
        drain(s1.at[n], ss1.at[n])
    send_straight(2, 0)
    send_straight(3, 0)
    send_straight(2, 1)
    send_straight(3, 1)
    send_straight_late(0, 0)
    send_straight_late(0, 1)
    send_z(2, 0)
    send_z(3, 0)
    send_straight_late(1, 0)
    send_straight_late(1, 1)
    send_z(2, 1)
    send_z(3, 1)
    for n in range(2):
        drain(s1.at[n + 2], ss1.at[n + 2])
        for part in range(2):
            finish(n, part)
            sent(n, part)
    finish(2, 0)
    finish(3, 0)
    finish(2, 1)
    finish(3, 1)
    for n in range(2, 4):
        for part in range(2):
            sent(n, part)


def body(pulses, steering, merge_re, merge_im, range_shift, image_map):
    vmem = pl.BlockSpec(memory_space=pltpu.VMEM)
    dma = pltpu.SemaphoreType.DMA
    return pl.pallas_call(
        kernel,
        out_shape=pltpu.VMEM((16, 1024), F32),
        in_specs=[pl.BlockSpec(memory_space=pltpu.HBM)] * 6,
        out_specs=vmem,
        scratch_shapes=[
            pltpu.VMEM((2, 128, 128), BF16),
            pltpu.VMEM((3, 256, 256), BF16),
            pltpu.VMEM((3, 256, 256), BF16),
            pltpu.VMEM((3, 2, 128), jnp.int32),
            pltpu.VMEM((256, 512), BF16),
            pltpu.VMEM((2, 8, 768, 128), BF16),
            pltpu.VMEM((128, 256), BF16),
            pltpu.VMEM((512, 512), BF16),
            pltpu.VMEM((256, 512), BF16),
            pltpu.VMEM((256, 512), BF16),
            pltpu.VMEM((2, 2, 656, 128), F32),
            pltpu.VMEM((320, 512), F32),
            pltpu.VMEM((288, 512), F32),
            pltpu.VMEM((272, 1024), F32),
            pltpu.VMEM((2, 4, 4, 2, 32, 1024), BF16),
            pltpu.VMEM((4, 256, 128), BF16),
            pltpu.VMEM((4, 2, 256, 128), BF16),
            pltpu.VMEM((4, 4, 256, 128), BF16),
            pltpu.VMEM((4, 1024, WIDTH), BF16),
            pltpu.VMEM((4, 2, 256, WIDTH), F32),
            pltpu.VMEM((4, 2, 2, 2, 2, 32, WIDTH), F32),
            pltpu.VMEM((4, 6, 2, 256, 128), BF16),
            pltpu.VMEM((4, 6, 2, 256, 128), BF16),
            pltpu.VMEM((4, 2, 3, 128, 128), BF16),
            pltpu.VMEM((4, 2, 3, 128, 128), BF16),
            pltpu.VMEM((4, 2, 3, 16, 128), BF16),
            pltpu.VMEM((4, 2, 3, 16, 128), BF16),
            pltpu.VMEM((4, 2, 8, 16, 128), BF16),
            pltpu.VMEM((4, 2, 8, 16, 128), BF16),
            pltpu.VMEM((4, 2, 8, 4, 16, 128), BF16),
            pltpu.VMEM((4, 2, 8, 4, 16, 128), BF16),
            pltpu.VMEM((4, 2, 4, 16, 128), F32),
            dma((5,)),
            dma((8,)),
            dma((1,)),
            dma((8,)),
            dma((2,)),
            dma((4, 3)),
            dma((1,)),
            dma((4,)),
            dma((4,)),
            dma((4, 4)),
            dma((4, 2)),
            dma((4, 2)),
            dma((4, 2)),
            dma((4, 2)),
            pltpu.SemaphoreType.REGULAR((4,)),
        ],
        compiler_params=pltpu.CompilerParams(
            collective_id=0, has_side_effects=True, vmem_limit_bytes=66_000_000
        ),
        cost_estimate=pl.CostEstimate(flops=8_000_000_000, bytes_accessed=6_000_000, transcendentals=0),
        name="window",
    )(
        pulses.reshape(-1, pulses.shape[2]),
        steering,
        merge_re,
        merge_im,
        range_shift,
        image_map.reshape(256, 512),
    )


def solution(mesh):
    placed = (
        P(None, None, ("pulse", "tile")),
        P(),
        P(),
        P(),
        P(),
        P("pulse", "tile", None, None, None),
    )
    return jax.shard_map(
        body, mesh=mesh, in_specs=placed, out_specs=P(("pulse", "tile"), None), check_vma=False
    )
```
